512 devices in a mesh: row: 64 (over y, z), col: 8 (over x, core).
Axes of the slice: x: 4, y: 4, z: 16, core: 2. Of those that a mesh axis runs over, the one named last changes fastest.
Arguments:
- sources: bfloat16 [524288, 640], P(('row', 'col')), may hold values from -6 to 6
- tree_perm: int32 [524288], P(('row', 'col')), may hold values from 0 to 524287, as said below
- leaf_blocks: bfloat16 [524288, 512], P(('row', 'col')), may hold values from -0.25 to 0.25
- u_factors: bfloat16 [10, 32, 524288], P(None, None, ('row', 'col')), may hold values from -0.3125 to 0.3125
- v_factors: bfloat16 [10, 32, 524288], P(None, None, ('row', 'col')), as said below
- level_ranks: int32 [10], replicated, may hold values from 16 to 32
Outputs:
- products: bfloat16 [524288, 640], P(('row', 'col'))
The draws below stay inside these ranges and needn't reach their ends.
Inputs may be any that keep to these rules, and one draw needn't show every extreme that they name: tree_perm is a permutation that maps each aligned block of 1024 positions onto the same block of initial indices. `v_factors`: entries of level l are of the order of the inverse square root of 524288 / 2^l.
All inputs are finite; a program needn't handle non-finite values.
Results may differ from the reference program's by a relative error of at most 0.0037.
Values sent between devices are 32-bit elements; how exact they have to be, the bound alone decides.
No kernel may reach another device: no remote copies, remote signals or barrier semaphores. Data moves between devices by JAX's collectives and lax.ppermute only.
A program may use at most 64 MiB of HBM per device.

```python
import jax
import jax.numpy as jnp
from jax import lax

LEAF = 512
K = 32
RHS = 640
ROWS_DEV = 1024
N = 524288
LEVELS = 10


def draw_tree_perm(key, part):
    blocks = N // ROWS_DEV
    keys = jax.random.split(key, blocks)
    perms = jax.vmap(lambda one_key: jax.random.permutation(one_key, ROWS_DEV))(keys).astype(jnp.int32)
    offsets = jnp.arange(blocks, dtype=jnp.int32)[:, None] * ROWS_DEV
    return (perms + offsets).reshape(N).astype(jnp.int32)


def draw_v_factors(key, part):
    level_scale = jnp.sqrt(2.0 ** (jnp.arange(LEVELS, dtype=jnp.float32) + 1.0) / N)
    base = jax.random.normal(key, (LEVELS, K, N), jnp.float32)
    return (base * level_scale[:, None, None]).astype(jnp.bfloat16)


def set_ends(array, stream_key, low, top_value):
    shape = array.shape
    place = [jax.random.randint(jax.random.fold_in(stream_key, axis), (), 0, shape[axis]) for axis in range(len(shape))]
    array = array.at[tuple(place)].set(low)
    longest = shape.index(max(shape))
    place[longest] = (place[longest] + 1) % shape[longest]
    return array.at[tuple(place)].set(top_value)


def levels(rng, extent, cuts, smallest, largest):
    level = 1.0
    for dim, blocks in cuts:
        steps = jax.random.uniform(jax.random.fold_in(jax.random.fold_in(rng, 6), dim), (blocks,), jnp.float32, smallest / len(cuts), largest / len(cuts))
        level = level * jnp.repeat(jnp.exp(steps), extent[dim] // blocks).reshape((-1,) + (1,) * (len(extent) - 1 - dim))
    return level


def bell_draw(stream_key, shape, width, most, cuts=(), held_as=jnp.bfloat16):
    array = width * jax.random.normal(stream_key, shape, jnp.float32)
    if cuts:
        array = array * levels(stream_key, shape, cuts, -0.22, 0.18)
    return jnp.clip(array, -most, most).astype(held_as)


def setup_inputs(seed: int = 0) -> dict:
    arg_keys = jax.random.split(jax.random.key(seed), 7)
    return {
        "sources": bell_draw(arg_keys[0], (N, RHS), 1.0, 6.0, ((0, 512),)),
        "tree_perm": draw_tree_perm(jax.random.fold_in(arg_keys[6], 71), 0),
        "leaf_blocks": bell_draw(arg_keys[2], (N, LEAF), LEAF ** -0.5, 0.25, ((0, 512),)),
        "u_factors": bell_draw(arg_keys[3], (LEVELS, K, N), (K * LEVELS) ** -0.5, 0.3125, ((2, 512),)),
        "v_factors": draw_v_factors(jax.random.fold_in(arg_keys[6], 71), 0),
        "level_ranks": set_ends(jax.random.randint(arg_keys[5], (LEVELS,), K // 2, K + 1), jax.random.fold_in(arg_keys[5], 1), K // 2, K).astype(jnp.int32),
    }


def reference(sources, tree_perm, leaf_blocks, u_factors, v_factors, level_ranks):
    ordered = sources[tree_perm].astype(jnp.float32)
    leaf_count = N // LEAF
    result = jnp.einsum("gij,gjr->gir", leaf_blocks.reshape(leaf_count, LEAF, LEAF).astype(jnp.float32), ordered.reshape(leaf_count, LEAF, RHS)).reshape(N, RHS)
    rank_index = lax.iota(jnp.int32, K)
    for level in range(LEVELS):
        groups = 2 ** (level + 1)
        cluster_rows = N // groups
        v_level = v_factors[level].astype(jnp.float32).reshape(K, groups, cluster_rows)
        coef = jnp.einsum("kgs,gsr->gkr", v_level, ordered.reshape(groups, cluster_rows, RHS))
        far_coef = coef.reshape(groups // 2, 2, K, RHS)[:, ::-1].reshape(groups, K, RHS)
        rank_mask = (rank_index < level_ranks[level]).astype(jnp.float32)
        far_coef = (far_coef * rank_mask[None, :, None]).astype(jnp.bfloat16).astype(jnp.float32)
        u_level = u_factors[level].astype(jnp.float32).reshape(K, groups, cluster_rows)
        result = result + jnp.einsum("kgs,gkr->gsr", u_level, far_coef).reshape(N, RHS)
    tree_out = result.astype(jnp.bfloat16)
    return jnp.zeros((N, RHS), jnp.bfloat16).at[tree_perm].set(tree_out)
```

```python
import jax
import jax.numpy as jnp
from jax import lax
from jax.experimental import pallas as pl
from jax.experimental.pallas import tpu as pltpu
from jax.sharding import Mesh
from jax.sharding import PartitionSpec as P

AXES = ("y", "zh", "zl", "x", "c")
F32 = jnp.float32
BF16 = jnp.bfloat16
NN = (((1,), (0,)), ((), ()))
NT = (((1,), (1,)), ((), ()))


def dot(a, b, dims=NN):
    return lax.dot_general(a, b, dims, preferred_element_type=F32)


def one_hot_t(perm, first, count):
    n = perm.shape[1]
    j = lax.broadcasted_iota(jnp.int32, (count, n), 0) + first
    return jnp.where(j == perm, 1.0, 0.0).astype(BF16)


def coef_kernel(core, perm_ref, v_ref, s_ref, mine_ref, send_ref, acc):
    n = s_ref.shape[0]
    rank = v_ref.shape[1]
    perm = perm_ref[...] & (n - 1)
    v = v_ref[0:9].reshape(9 * rank, n)
    step = 256
    total = None
    for j in range(0, n, step):
        vp = dot(v, one_hot_t(perm, j, step), NT).astype(BF16)
        part = dot(vp, s_ref[j : j + step, :])
        total = part if total is None else total + part
    half = 4 * rank
    me = core[0]
    mine = pl.ds(pl.multiple_of(me * half, half), half)
    theirs = pl.ds(pl.multiple_of((1 - me) * half, half), half)
    for d in range(acc.shape[0]):
        lanes = slice(d * 128, (d + 1) * 128)
        for level in range(8):
            acc[d, pl.ds(level, rank, stride=8), :] = total[level * rank : (level + 1) * rank, lanes]
        mine_ref[:, lanes] = acc[d, mine, :]
        send_ref[0:half, lanes] = acc[d, theirs, :]
    send_ref[half : half + rank, :] = total[8 * rank : 9 * rank]


def local_kernel(ranks, perm_ref, s_ref, leaf_ref, u_ref, v_ref, near_ref, base_ref, ut_ref, p_ref, pt_ref, ord_ref, lp_ref, uf_ref, us_ref, ue_ref, fe_ref):
    n, _ = s_ref.shape
    leaf = leaf_ref.shape[1]
    rank = u_ref.shape[1]
    perm = perm_ref[...] & (n - 1)
    step = 256
    for j in range(0, n, step):
        pt_ref[j : j + step, :] = one_hot_t(perm, j, step)
    for i in range(0, n, 128):
        column = jnp.broadcast_to(perm[:, i : i + 128], (128, 128)).T
        lane = lax.broadcasted_iota(jnp.int32, (128, 128), 1)
        for j in range(0, n, 128):
            p_ref[i : i + 128, j : j + 128] = jnp.where(column == lane + j, 1.0, 0.0).astype(BF16)

    row = lax.broadcasted_iota(jnp.int32, (rank, n), 0)
    lane_n = lax.broadcasted_iota(jnp.int32, (rank, n), 1)
    for level in range(8):
        kept = jnp.where(row < ranks[level], u_ref[level].astype(F32), 0.0)
        for d in range(n // 128):
            uf_ref[d, pl.ds(level, rank, stride=8), :] = kept[:, d * 128 : (d + 1) * 128]
    for d in range(n // 128):
        us_ref[:, d * 128 : (d + 1) * 128] = uf_ref[d].astype(BF16)
    ue_ref[0:rank, :] = jnp.where(row < ranks[8], u_ref[8].astype(F32), 0.0).astype(BF16)
    last = jnp.where(row < ranks[9], u_ref[9].astype(F32), 0.0)
    ue_ref[rank : 2 * rank, :] = jnp.where(lane_n < leaf, last, 0.0).astype(BF16)
    ue_ref[2 * rank : 3 * rank, :] = jnp.where(lane_n < leaf, 0.0, last).astype(BF16)

    def order(b, _):
        rows = pl.ds(pl.multiple_of(b * step, step), step)
        ord_ref[rows, :] = dot(p_ref[rows, :], s_ref[...]).astype(BF16)
        for g in range(0, n, leaf):
            lp_ref[rows, g : g + leaf] = dot(pt_ref[rows, g : g + leaf], leaf_ref[g : g + leaf, :]).astype(BF16)
        ut_ref[rows, :] = dot(pt_ref[rows, :], us_ref[...], NT).astype(BF16)
        return 0

    lax.fori_loop(0, n // step, order, 0)
    fe_ref[0:rank, :] = near_ref[...].astype(BF16)
    fe_ref[rank : 2 * rank, :] = dot(v_ref[9][:, leaf:], ord_ref[leaf:, :]).astype(BF16)
    fe_ref[2 * rank : 3 * rank, :] = dot(v_ref[9][:, :leaf], ord_ref[:leaf, :]).astype(BF16)

    def apply(b, _):
        rows = pl.ds(pl.multiple_of(b * step, step), step)
        ue = dot(pt_ref[rows, :], ue_ref[...], NT).astype(BF16)
        base_ref[rows, :] = dot(lp_ref[rows, :], ord_ref[...]) + dot(ue, fe_ref[...])
        return 0

    lax.fori_loop(0, n // step, apply, 0)


def level_row(place, p):
    y, zh = place[0], place[1]
    py, pz = p // 4, p % 4
    same = jnp.where(pz == (zh ^ 1), 3, 2)
    return jnp.where(py == y, same, jnp.where(py == (y ^ 1), 1, 0))


def middle_kernel(place, got_ref, out_ref, fine_ref, tot_ref):
    row = lax.broadcasted_iota(jnp.int32, got_ref.shape[1:], 0)
    got = lambda zl, x: got_ref[zl * 4 + x]
    sums = [(got(zl, 0) + got(zl, 1)) + (got(zl, 2) + got(zl, 3)) for zl in range(4)]
    tot_ref[...] = (sums[0] + sums[1]) + (sums[2] + sums[3])
    for zl in range(4):
        low = jnp.where(row == 5, sums[zl ^ 1], sums[zl ^ 2] + sums[zl ^ 3])
        for x in range(4):
            high = jnp.where(row == 7, got(zl, x ^ 1), got(zl, x ^ 2) + got(zl, x ^ 3))
            fine_ref[zl * 4 + x] = jnp.where(row >= 6, high, low)
    for p in range(16):
        out_ref[p] = tot_ref[pl.ds(level_row(place, p), 1), :]


def far_kernel(place, got_ref, fine_ref, out_ref, acc):
    acc[...] = jnp.zeros_like(acc)
    me = place[0] * 4 + place[1]
    for p in range(16):
        at = pl.ds(level_row(place, p), 1)
        acc[at, :] = acc[at, :] + jnp.where(me == p, 0.0, got_ref[p])
    row = lax.broadcasted_iota(jnp.int32, acc.shape, 0)
    far = acc[...]
    for p in range(16):
        out_ref[p] = jnp.where(row < 4, far, fine_ref[p])


def last_kernel(far_ref, ut_ref, base_ref, out_ref, far16):
    @pl.when(pl.program_id(0) == 0)
    def _():
        far16[...] = far_ref[...].astype(BF16)

    out_ref[...] = (base_ref[...] + dot(ut_ref[...], far16[...])).astype(BF16)


SMEM = pl.BlockSpec(memory_space=pltpu.SMEM)
VMEM = pl.BlockSpec(memory_space=pltpu.VMEM)


def shape(dims, dtype=F32):
    return jax.ShapeDtypeStruct(dims, dtype)


def per_device(sources, tree_perm, leaf_blocks, u_factors, v_factors, level_ranks):
    n, rhs = sources.shape
    rank = u_factors.shape[1]
    half = 4 * rank
    core = lax.axis_index("c")
    place = jnp.stack([lax.axis_index("y"), lax.axis_index("zh")])
    perm = tree_perm.reshape(1, n)
    mine, send = pl.pallas_call(
        coef_kernel,
        name="coef",
        in_specs=[SMEM, VMEM, VMEM, VMEM],
        out_specs=[VMEM, VMEM],
        out_shape=[shape((half, rhs)), shape((half + rank, rhs))],
        scratch_shapes=[pltpu.VMEM((rhs // 128, 2 * half, 128), F32)],
    )(core.reshape(1), perm, v_factors, sources)
    pair = lax.all_gather(send, "c")
    other = lax.dynamic_index_in_dim(pair, 1 - core, 0, keepdims=False)
    near = other[half:]
    partial = (mine + other[:half]).reshape(16, 8, rhs)
    base, ut = pl.pallas_call(
        local_kernel,
        name="local",
        in_specs=[SMEM] + [VMEM] * 6,
        out_specs=[VMEM, VMEM],
        out_shape=[shape((n, rhs)), shape((n, 2 * half), BF16)],
        scratch_shapes=[
            pltpu.VMEM((n, n), BF16),
            pltpu.VMEM((n, n), BF16),
            pltpu.VMEM((n, rhs), BF16),
            pltpu.VMEM((n, n), BF16),
            pltpu.VMEM((n // 128, 2 * half, 128), F32),
            pltpu.VMEM((2 * half, n), BF16),
            pltpu.VMEM((3 * rank, n), BF16),
            pltpu.VMEM((3 * rank, rhs), BF16),
        ],
        cost_estimate=pl.CostEstimate(flops=4_600_000_000, bytes_accessed=8_000_000, transcendentals=0),
    )(level_ranks, perm, sources, leaf_blocks, u_factors, v_factors, near)
    got = lax.all_to_all(partial, ("zl", "x"), 0, 0, tiled=True)
    rows, fine = pl.pallas_call(
        middle_kernel,
        name="middle",
        in_specs=[SMEM, VMEM],
        out_specs=[VMEM, VMEM],
        out_shape=[shape((16, 1, rhs)), shape((16, 8, rhs))],
        scratch_shapes=[pltpu.VMEM((8, rhs), F32)],
    )(place, got)
    rows = lax.all_to_all(rows, ("y", "zh"), 0, 0, tiled=True)
    far = pl.pallas_call(
        far_kernel,
        name="far",
        in_specs=[SMEM, VMEM, VMEM],
        out_specs=VMEM,
        out_shape=shape((16, 8, rhs)),
        scratch_shapes=[pltpu.VMEM((8, rhs), F32)],
    )(place, rows, fine)
    far = lax.all_to_all(far, ("zl", "x"), 0, 0, tiled=True)
    far = lax.all_gather(far.reshape(half, rhs), "c", axis=0, tiled=True)
    step = 256
    return pl.pallas_call(
        last_kernel,
        name="last",
        grid=(n // step,),
        in_specs=[
            pl.BlockSpec((2 * half, rhs), lambda i: (0, 0)),
            pl.BlockSpec((step, 2 * half), lambda i: (i, 0)),
            pl.BlockSpec((step, rhs), lambda i: (i, 0)),
        ],
        out_specs=pl.BlockSpec((step, rhs), lambda i: (i, 0)),
        out_shape=shape((n, rhs), BF16),
        scratch_shapes=[pltpu.VMEM((2 * half, rhs), BF16)],
    )(far, ut, base)


def solution(mesh):
    torus = Mesh(mesh.devices.reshape(4, 4, 4, 4, 2), AXES)
    placed = (P(AXES, None), P(AXES), P(AXES, None), P(None, None, AXES), P(None, None, AXES), P())
    return jax.shard_map(
        per_device, mesh=torus, in_specs=placed, out_specs=P(AXES, None), check_vma=False
    )
```

```python
import jax
import jax.numpy as jnp
from jax import lax
from jax.experimental import pallas as pl
from jax.experimental.pallas import tpu as pltpu
from jax.sharding import Mesh
from jax.sharding import PartitionSpec as P

AXES = ("y", "zh", "zl", "x", "c")
F32 = jnp.float32
BF16 = jnp.bfloat16
NN = (((1,), (0,)), ((), ()))
NT = (((1,), (1,)), ((), ()))


def dot(a, b, dims=NN):
    return lax.dot_general(a, b, dims, preferred_element_type=F32)


def one_hot_t(perm, first, count):
    n = perm.shape[1]
    j = lax.broadcasted_iota(jnp.int32, (count, n), 0) + first
    return jnp.where(j == perm, 1.0, 0.0).astype(BF16)


def coef_kernel(core, perm_ref, v_hbm, s_hbm, mine_ref, send_ref, acc, v_ref, s_ref, v_sem, s_sem):
    n = s_ref.shape[0]
    levels, rank, _ = v_ref.shape
    step = 256
    v_copy = pltpu.make_async_copy(v_hbm.at[0:levels], v_ref, v_sem)
    v_copy.start()
    s_copy = [
        pltpu.make_async_copy(s_hbm.at[j : j + step], s_ref.at[j : j + step], s_sem.at[j // step])
        for j in range(0, n, step)
    ]
    for copy in s_copy:
        copy.start()
    perm = perm_ref[...] & (n - 1)
    hot = one_hot_t(perm, 0, step)
    v_copy.wait()
    v = v_ref[...].reshape(levels * rank, n)
    total = None
    for j in range(0, n, step):
        vp = dot(v, hot, NT).astype(BF16)
        if j + step < n:
            hot = one_hot_t(perm, j + step, step)
        s_copy[j // step].wait()
        part = dot(vp, s_ref[j : j + step, :])
        total = part if total is None else total + part
    half = 4 * rank
    me = core[0]
    mine = pl.ds(pl.multiple_of(me * half, half), half)
    theirs = pl.ds(pl.multiple_of((1 - me) * half, half), half)
    for d in range(acc.shape[0]):
        lanes = slice(d * 128, (d + 1) * 128)
        for level in range(8):
            acc[d, pl.ds(level, rank, stride=8), :] = total[level * rank : (level + 1) * rank, lanes]
        mine_ref[:, lanes] = acc[d, mine, :]
        send_ref[0:half, lanes] = acc[d, theirs, :]
    send_ref[half : half + rank, :] = total[8 * rank : 9 * rank]


def local_kernel(ranks, core, perm_ref, s_ref, leaf_ref, u_ref, v_ref, pair_ref, _, base_ref, ut_ref, p_ref, pt_ref, ord_ref, lp_ref, uf_ref, us_ref, ue_ref, fe_ref):
    n, _ = s_ref.shape
    leaf = leaf_ref.shape[1]
    rank = u_ref.shape[1]
    perm = perm_ref[...] & (n - 1)
    step = 256
    for j in range(0, n, step):
        pt_ref[j : j + step, :] = one_hot_t(perm, j, step)
    for i in range(0, n, 128):
        column = jnp.broadcast_to(perm[:, i : i + 128], (128, 128)).T
        lane = lax.broadcasted_iota(jnp.int32, (128, 128), 1)
        for j in range(0, n, 128):
            p_ref[i : i + 128, j : j + 128] = jnp.where(column == lane + j, 1.0, 0.0).astype(BF16)

    row = lax.broadcasted_iota(jnp.int32, (rank, n), 0)
    lane_n = lax.broadcasted_iota(jnp.int32, (rank, n), 1)
    for level in range(8):
        kept = jnp.where(row < ranks[level], u_ref[level].astype(F32), 0.0)
        for d in range(n // 128):
            uf_ref[d, pl.ds(level, rank, stride=8), :] = kept[:, d * 128 : (d + 1) * 128]
    for d in range(n // 128):
        us_ref[:, d * 128 : (d + 1) * 128] = uf_ref[d].astype(BF16)
    ue_ref[0:rank, :] = jnp.where(row < ranks[8], u_ref[8].astype(F32), 0.0).astype(BF16)
    last = jnp.where(row < ranks[9], u_ref[9].astype(F32), 0.0)
    ue_ref[rank : 2 * rank, :] = jnp.where(lane_n < leaf, last, 0.0).astype(BF16)
    ue_ref[2 * rank : 3 * rank, :] = jnp.where(lane_n < leaf, 0.0, last).astype(BF16)

    def order(b, _):
        rows = pl.ds(pl.multiple_of(b * step, step), step)
        ord_ref[rows, :] = dot(p_ref[rows, :], s_ref[...]).astype(BF16)
        for g in range(0, n, leaf):
            lp_ref[rows, g : g + leaf] = dot(pt_ref[rows, g : g + leaf], leaf_ref[g : g + leaf, :]).astype(BF16)
        ut_ref[rows, :] = dot(pt_ref[rows, :], us_ref[...], NT).astype(BF16)
        return 0

    lax.fori_loop(0, n // step, order, 0)
    fe_ref[0:rank, :] = pair_ref[1 - core[0], 4 * rank :, :].astype(BF16)
    fe_ref[rank : 2 * rank, :] = dot(v_ref[9][:, leaf:], ord_ref[leaf:, :]).astype(BF16)
    fe_ref[2 * rank : 3 * rank, :] = dot(v_ref[9][:, :leaf], ord_ref[:leaf, :]).astype(BF16)

    def apply(b, _):
        rows = pl.ds(pl.multiple_of(b * step, step), step)
        ue = dot(pt_ref[rows, :], ue_ref[...], NT).astype(BF16)
        base_ref[rows, :] = dot(lp_ref[rows, :], ord_ref[...]) + dot(ue, fe_ref[...])
        return 0

    lax.fori_loop(0, n // step, apply, 0)


def level_row(place, p):
    y, zh = place[0], place[1]
    py, pz = p // 4, p % 4
    same = jnp.where(pz == (zh ^ 1), 3, 2)
    return jnp.where(py == y, same, jnp.where(py == (y ^ 1), 1, 0))


def middle_kernel(place, got_ref, out_ref, fine_ref, tot_ref):
    row = lax.broadcasted_iota(jnp.int32, got_ref.shape[1:], 0)
    got = lambda zl, x: got_ref[zl * 4 + x]
    sums = [(got(zl, 0) + got(zl, 1)) + (got(zl, 2) + got(zl, 3)) for zl in range(4)]
    tot_ref[...] = (sums[0] + sums[1]) + (sums[2] + sums[3])
    for zl in range(4):
        low = jnp.where(row == 5, sums[zl ^ 1], sums[zl ^ 2] + sums[zl ^ 3])
        for x in range(4):
            high = jnp.where(row == 7, got(zl, x ^ 1), got(zl, x ^ 2) + got(zl, x ^ 3))
            fine_ref[zl * 4 + x] = jnp.where(row >= 6, high, low)
    for p in range(16):
        out_ref[p] = tot_ref[pl.ds(level_row(place, p), 1), :]


def far_kernel(place, got_ref, fine_ref, _, out_ref, acc):
    acc[...] = jnp.zeros_like(acc)
    me = place[0] * 4 + place[1]
    for p in range(16):
        at = pl.ds(level_row(place, p), 1)
        acc[at, :] = acc[at, :] + jnp.where(me == p, 0.0, got_ref[p])
    row = lax.broadcasted_iota(jnp.int32, acc.shape, 0)
    far = acc[...]
    for p in range(16):
        out_ref[p] = jnp.where(row < 4, far, fine_ref[p])


def last_kernel(far_ref, ut_ref, base_ref, out_ref, far16):
    @pl.when(pl.program_id(0) == 0)
    def _():
        far16[...] = far_ref[...].astype(BF16)

    out_ref[...] = (base_ref[...] + dot(ut_ref[...], far16[...])).astype(BF16)


SMEM = pl.BlockSpec(memory_space=pltpu.SMEM)
VMEM = pl.BlockSpec(memory_space=pltpu.VMEM)
ANY = pl.BlockSpec(memory_space=pl.ANY)


def grant(mib):
    return pltpu.CompilerParams(vmem_limit_bytes=mib << 20)


def shape(dims, dtype=F32):
    return jax.ShapeDtypeStruct(dims, dtype)


def per_device(sources, tree_perm, leaf_blocks, u_factors, v_factors, level_ranks):
    n, rhs = sources.shape
    rank = u_factors.shape[1]
    half = 4 * rank
    core = lax.axis_index("c").reshape(1)
    place = jnp.stack([lax.axis_index("y"), lax.axis_index("zh")])
    perm = tree_perm.reshape(1, n)
    mine, send = pl.pallas_call(
        coef_kernel,
        name="coef",
        in_specs=[SMEM, VMEM, ANY, ANY],
        out_specs=[VMEM, VMEM],
        out_shape=[shape((half, rhs)), shape((half + rank, rhs))],
        scratch_shapes=[
            pltpu.VMEM((rhs // 128, 2 * half, 128), F32),
            pltpu.VMEM((9, rank, n), BF16),
            pltpu.VMEM((n, rhs), BF16),
            pltpu.SemaphoreType.DMA,
            pltpu.SemaphoreType.DMA((n // 256,)),
        ],
        compiler_params=grant(14),
    )(core, perm, v_factors, sources)
    pair = lax.all_gather(send, "c")
    other = lax.dynamic_index_in_dim(pair, 1 - core[0], 0, keepdims=False)
    partial = (mine + other[:half]).reshape(16, 8, rhs)
    got = lax.all_to_all(partial, ("zl", "x"), 0, 0, tiled=True)
    rows, fine = pl.pallas_call(
        middle_kernel,
        name="middle",
        in_specs=[SMEM, VMEM],
        out_specs=[VMEM, VMEM],
        out_shape=[shape((16, 1, rhs)), shape((16, 8, rhs))],
        scratch_shapes=[pltpu.VMEM((8, rhs), F32)],
        compiler_params=grant(4),
    )(place, got)
    base, ut = pl.pallas_call(
        local_kernel,
        name="local",
        in_specs=[SMEM, SMEM] + [VMEM] * 6 + [ANY],
        out_specs=[VMEM, VMEM],
        out_shape=[shape((n, rhs)), shape((n, 2 * half), BF16)],
        scratch_shapes=[
            pltpu.VMEM((n, n), BF16),
            pltpu.VMEM((n, n), BF16),
            pltpu.VMEM((n, rhs), BF16),
            pltpu.VMEM((n, n), BF16),
            pltpu.VMEM((n // 128, 2 * half, 128), F32),
            pltpu.VMEM((2 * half, n), BF16),
            pltpu.VMEM((3 * rank, n), BF16),
            pltpu.VMEM((3 * rank, rhs), BF16),
        ],
        compiler_params=grant(32),
        cost_estimate=pl.CostEstimate(flops=4_600_000_000, bytes_accessed=8_000_000, transcendentals=0),
    )(level_ranks, core, perm, sources, leaf_blocks, u_factors, v_factors, pair, fine)
    rows = lax.all_to_all(rows, ("y", "zh"), 0, 0, tiled=True)
    far = pl.pallas_call(
        far_kernel,
        name="far",
        in_specs=[SMEM, VMEM, VMEM, ANY],
        out_specs=VMEM,
        out_shape=shape((16, 8, rhs)),
        scratch_shapes=[pltpu.VMEM((8, rhs), F32)],
        compiler_params=grant(4),
    )(place, rows, fine, ut)
    far = lax.all_to_all(far, ("zl", "x"), 0, 0, tiled=True)
    far = lax.all_gather(far.reshape(half, rhs), "c", axis=0, tiled=True)
    step = 256
    return pl.pallas_call(
        last_kernel,
        name="last",
        grid=(n // step,),
        in_specs=[
            pl.BlockSpec((2 * half, rhs), lambda i: (0, 0)),
            pl.BlockSpec((step, 2 * half), lambda i: (i, 0)),
            pl.BlockSpec((step, rhs), lambda i: (i, 0)),
        ],
        out_specs=pl.BlockSpec((step, rhs), lambda i: (i, 0)),
        out_shape=shape((n, rhs), BF16),
        scratch_shapes=[pltpu.VMEM((2 * half, rhs), BF16)],
        compiler_params=grant(8),
    )(far, ut, base)


def solution(mesh):
    torus = Mesh(mesh.devices.reshape(4, 4, 4, 4, 2), AXES)
    placed = (P(AXES, None), P(AXES), P(AXES, None), P(None, None, AXES), P(None, None, AXES), P())
    return jax.shard_map(
        per_device, mesh=torus, in_specs=placed, out_specs=P(AXES, None), check_vma=False
    )
```

```python
import jax
import jax.numpy as jnp
from jax import lax
from jax.experimental import pallas as pl
from jax.experimental.pallas import tpu as pltpu
from jax.sharding import Mesh
from jax.sharding import PartitionSpec as P

AXES = ("y", "zh", "zl", "x", "c")
F32 = jnp.float32
BF16 = jnp.bfloat16
NN = (((1,), (0,)), ((), ()))
NT = (((1,), (1,)), ((), ()))


def dot(a, b, dims=NN):
    return lax.dot_general(a, b, dims, preferred_element_type=F32)


def one_hot_t(perm, first, count):
    n = perm.shape[1]
    j = lax.broadcasted_iota(jnp.int32, (count, n), 0) + first
    return jnp.where(j == perm, 1.0, 0.0).astype(BF16)


def coef_kernel(core, perm_hbm, v_hbm, s_hbm, mine_ref, send_ref, acc, perm_ref, v_ref, s_ref, perm_sem, v_sem, s_sem):
    n = s_ref.shape[0]
    levels, rank, _ = v_ref.shape
    step = 256
    perm_copy = pltpu.make_async_copy(perm_hbm, perm_ref, perm_sem)
    perm_copy.start()
    v_copy = pltpu.make_async_copy(v_hbm.at[0:levels], v_ref, v_sem)
    v_copy.start()
    s_copy = [
        pltpu.make_async_copy(s_hbm.at[j : j + step], s_ref.at[j : j + step], s_sem.at[j // step])
        for j in range(0, n, step)
    ]
    for copy in s_copy:
        copy.start()
    perm_copy.wait()
    perm = perm_ref[...] & (n - 1)
    hot = one_hot_t(perm, 0, step)
    v_copy.wait()
    v = v_ref[...].reshape(levels * rank, n)
    total = None
    for j in range(0, n, step):
        vp = dot(v, hot, NT).astype(BF16)
        if j + step < n:
            hot = one_hot_t(perm, j + step, step)
        s_copy[j // step].wait()
        part = dot(vp, s_ref[j : j + step, :])
        total = part if total is None else total + part
    half = 4 * rank
    me = core[0]
    mine = pl.ds(pl.multiple_of(me * half, half), half)
    theirs = pl.ds(pl.multiple_of((1 - me) * half, half), half)
    for d in range(acc.shape[0]):
        lanes = slice(d * 128, (d + 1) * 128)
        for level in range(8):
            acc[d, pl.ds(level, rank, stride=8), :] = total[level * rank : (level + 1) * rank, lanes]
        mine_ref[:, lanes] = acc[d, mine, :]
        send_ref[0:half, lanes] = acc[d, theirs, :]
    send_ref[half : half + rank, :] = total[8 * rank : 9 * rank]


def local_kernel(
    ranks, core, perm_hbm, s_hbm, leaf_hbm, u_hbm, v_hbm, pair_ref, _,
    ord_hbm, lp_hbm, ut_ref, et_ref, fe_ref, token_ref,
    perm_ref, s_ref, leaf_ref, u_ref, v_ref, p_ref, pt_ref, uf_ref, us_ref, ue_ref, ord_ref, lp_ref, sems, ord_sems, lp_sems,
):
    n, _ = s_ref.shape
    leaf = leaf_ref.shape[1]
    rank = u_ref.shape[1]
    pairs = ((perm_hbm, perm_ref), (s_hbm, s_ref), (u_hbm, u_ref), (leaf_hbm, leaf_ref), (v_hbm.at[9], v_ref))
    copies = [pltpu.make_async_copy(a, b, sems.at[k]) for k, (a, b) in enumerate(pairs)]
    for copy in copies:
        copy.start()
    copies[0].wait()
    perm = perm_ref[...] & (n - 1)
    step = 256
    for j in range(0, n, step):
        pt_ref[j : j + step, :] = one_hot_t(perm, j, step)
    for i in range(0, n, 128):
        column = jnp.broadcast_to(perm[:, i : i + 128], (128, 128)).T
        lane = lax.broadcasted_iota(jnp.int32, (128, 128), 1)
        for j in range(0, n, 128):
            p_ref[i : i + 128, j : j + 128] = jnp.where(column == lane + j, 1.0, 0.0).astype(BF16)
    for copy in copies[1:]:
        copy.wait()

    row = lax.broadcasted_iota(jnp.int32, (rank, n), 0)
    lane_n = lax.broadcasted_iota(jnp.int32, (rank, n), 1)
    for level in range(8):
        kept = jnp.where(row < ranks[level], u_ref[level].astype(F32), 0.0)
        for d in range(n // 128):
            uf_ref[d, pl.ds(level, rank, stride=8), :] = kept[:, d * 128 : (d + 1) * 128]
    for d in range(n // 128):
        us_ref[:, d * 128 : (d + 1) * 128] = uf_ref[d].astype(BF16)
    ue_ref[0:rank, :] = jnp.where(row < ranks[8], u_ref[8].astype(F32), 0.0).astype(BF16)
    last = jnp.where(row < ranks[9], u_ref[9].astype(F32), 0.0)
    ue_ref[rank : 2 * rank, :] = jnp.where(lane_n < leaf, last, 0.0).astype(BF16)
    ue_ref[2 * rank : 3 * rank, :] = jnp.where(lane_n < leaf, 0.0, last).astype(BF16)

    def kept_copies(b):
        rows = pl.ds(pl.multiple_of(b * step, step), step)
        return (
            pltpu.make_async_copy(ord_ref.at[rows], ord_hbm.at[rows], ord_sems.at[b]),
            pltpu.make_async_copy(lp_ref.at[rows], lp_hbm.at[rows], lp_sems.at[b]),
        )

    def order(b, _):
        rows = pl.ds(pl.multiple_of(b * step, step), step)
        ord_ref[rows, :] = dot(p_ref[rows, :], s_ref[...]).astype(BF16)
        for g in range(0, n, leaf):
            lp_ref[rows, g : g + leaf] = dot(pt_ref[rows, g : g + leaf], leaf_ref[g : g + leaf, :]).astype(BF16)
        ut_ref[rows, :] = dot(pt_ref[rows, :], us_ref[...], NT).astype(BF16)
        for copy in kept_copies(b):
            copy.start()
        et_ref[rows, :] = dot(pt_ref[rows, :], ue_ref[...], NT).astype(BF16)
        return 0

    lax.fori_loop(0, n // step, order, 0)
    fe_ref[0:rank, :] = pair_ref[1 - core[0], 4 * rank :, :].astype(BF16)
    fe_ref[rank : 2 * rank, :] = dot(v_ref[:, leaf:], ord_ref[leaf:, :]).astype(BF16)
    fe_ref[2 * rank : 3 * rank, :] = dot(v_ref[:, :leaf], ord_ref[:leaf, :]).astype(BF16)
    token_ref[...] = jnp.zeros_like(token_ref)
    for b in range(n // step):
        for copy in kept_copies(b):
            copy.wait()


def base_kernel(ord_ref, lp_ref, et_ref, fe_ref, _, base_ref):
    base_ref[...] = dot(lp_ref[...], ord_ref[...]) + dot(et_ref[...], fe_ref[...])


def level_row(place, p):
    y, zh = place[0], place[1]
    py, pz = p // 4, p % 4
    same = jnp.where(pz == (zh ^ 1), 3, 2)
    return jnp.where(py == y, same, jnp.where(py == (y ^ 1), 1, 0))


def middle_kernel(place, got_ref, _, out_ref, fine_ref, tot_ref):
    row = lax.broadcasted_iota(jnp.int32, got_ref.shape[1:], 0)
    got = lambda zl, x: got_ref[zl * 4 + x]
    sums = [(got(zl, 0) + got(zl, 1)) + (got(zl, 2) + got(zl, 3)) for zl in range(4)]
    tot_ref[...] = (sums[0] + sums[1]) + (sums[2] + sums[3])
    for zl in range(4):
        low = jnp.where(row == 5, sums[zl ^ 1], sums[zl ^ 2] + sums[zl ^ 3])
        for x in range(4):
            high = jnp.where(row == 7, got(zl, x ^ 1), got(zl, x ^ 2) + got(zl, x ^ 3))
            fine_ref[zl * 4 + x] = jnp.where(row >= 6, high, low)
    for p in range(16):
        out_ref[p] = tot_ref[pl.ds(level_row(place, p), 1), :]


def far_kernel(place, got_ref, fine_ref, out_ref, acc):
    acc[...] = jnp.zeros_like(acc)
    me = place[0] * 4 + place[1]
    for p in range(16):
        at = pl.ds(level_row(place, p), 1)
        acc[at, :] = acc[at, :] + jnp.where(me == p, 0.0, got_ref[p])
    row = lax.broadcasted_iota(jnp.int32, acc.shape, 0)
    far = acc[...]
    for p in range(16):
        out_ref[p] = jnp.where(row < 4, far, fine_ref[p])


def last_kernel(far_ref, ut_ref, base_ref, out_ref, far16):
    @pl.when(pl.program_id(0) == 0)
    def _():
        far16[...] = far_ref[...].astype(BF16)

    out_ref[...] = (base_ref[...] + dot(ut_ref[...], far16[...])).astype(BF16)


SMEM = pl.BlockSpec(memory_space=pltpu.SMEM)
VMEM = pl.BlockSpec(memory_space=pltpu.VMEM)
ANY = pl.BlockSpec(memory_space=pl.ANY)
HBM = pl.BlockSpec(memory_space=pltpu.HBM)


def grant(mib):
    return pltpu.CompilerParams(vmem_limit_bytes=mib << 20)


def in_hbm(*arrays):
    return [pltpu.with_memory_space_constraint(a, pltpu.HBM) for a in arrays]


def in_vmem(*arrays):
    return [pltpu.with_memory_space_constraint(a, pltpu.VMEM) for a in arrays]


def shape(dims, dtype=F32):
    return jax.ShapeDtypeStruct(dims, dtype)


def per_device(sources, tree_perm, leaf_blocks, u_factors, v_factors, level_ranks):
    n, rhs = sources.shape
    rank = u_factors.shape[1]
    half = 4 * rank
    core = lax.axis_index("c").reshape(1)
    place = jnp.stack([lax.axis_index("y"), lax.axis_index("zh")])
    perm = tree_perm.reshape(1, n)
    mine, send = pl.pallas_call(
        coef_kernel,
        name="coef",
        in_specs=[SMEM, HBM, HBM, HBM],
        out_specs=[VMEM, VMEM],
        out_shape=[shape((half, rhs)), shape((half + rank, rhs))],
        scratch_shapes=[
            pltpu.VMEM((rhs // 128, 2 * half, 128), F32),
            pltpu.VMEM((1, n), jnp.int32),
            pltpu.VMEM((9, rank, n), BF16),
            pltpu.VMEM((n, rhs), BF16),
            pltpu.SemaphoreType.DMA,
            pltpu.SemaphoreType.DMA,
            pltpu.SemaphoreType.DMA((n // 256,)),
        ],
        compiler_params=grant(14),
    )(core, *in_hbm(perm, v_factors, sources))
    pair = lax.all_gather(send, "c")
    other = lax.dynamic_index_in_dim(pair, 1 - core[0], 0, keepdims=False)
    partial = (mine + other[:half]).reshape(16, 8, rhs)
    ordered, leaves, ut, et, fe, token = pl.pallas_call(
        local_kernel,
        name="local",
        in_specs=[SMEM, SMEM] + [HBM] * 5 + [VMEM, ANY],
        out_specs=[HBM, HBM] + [VMEM] * 4,
        out_shape=[
            pltpu.HBM((n, rhs), BF16),
            pltpu.HBM((n, n), BF16),
            pltpu.VMEM((n, 2 * half), BF16),
            pltpu.VMEM((n, 3 * rank), BF16),
            pltpu.VMEM((3 * rank, rhs), BF16),
            shape((8, 128)),
        ],
        scratch_shapes=[
            pltpu.VMEM((1, n), jnp.int32),
            pltpu.VMEM((n, rhs), BF16),
            pltpu.VMEM(leaf_blocks.shape, BF16),
            pltpu.VMEM(u_factors.shape, BF16),
            pltpu.VMEM((rank, n), BF16),
            pltpu.VMEM((n, n), BF16),
            pltpu.VMEM((n, n), BF16),
            pltpu.VMEM((n // 128, 2 * half, 128), F32),
            pltpu.VMEM((2 * half, n), BF16),
            pltpu.VMEM((3 * rank, n), BF16),
            pltpu.VMEM((n, rhs), BF16),
            pltpu.VMEM((n, n), BF16),
            pltpu.SemaphoreType.DMA((5,)),
            pltpu.SemaphoreType.DMA((n // 256,)),
            pltpu.SemaphoreType.DMA((n // 256,)),
        ],
        compiler_params=grant(28),
        cost_estimate=pl.CostEstimate(flops=3_500_000_000, bytes_accessed=8_000_000, transcendentals=0),
    )(level_ranks, core, *in_hbm(perm, sources, leaf_blocks, u_factors, v_factors), *in_vmem(pair), partial)
    got = lax.all_to_all(partial, ("zl", "x"), 0, 0, tiled=True)
    rows, fine = pl.pallas_call(
        middle_kernel,
        name="middle",
        in_specs=[SMEM, VMEM, ANY],
        out_specs=[VMEM, VMEM],
        out_shape=[shape((16, 1, rhs)), shape((16, 8, rhs))],
        scratch_shapes=[pltpu.VMEM((8, rhs), F32)],
        compiler_params=grant(4),
    )(place, got, token)
    rows = lax.all_to_all(rows, ("y", "zh"), 0, 0, tiled=True)
    far = pl.pallas_call(
        far_kernel,
        name="far",
        in_specs=[SMEM, VMEM, VMEM],
        out_specs=VMEM,
        out_shape=shape((16, 8, rhs)),
        scratch_shapes=[pltpu.VMEM((8, rhs), F32)],
        compiler_params=grant(4),
    )(place, rows, fine)
    base = pl.pallas_call(
        base_kernel,
        name="base",
        grid=(n // 256,),
        in_specs=[
            pl.BlockSpec((n, rhs), lambda i: (0, 0)),
            pl.BlockSpec((256, n), lambda i: (i, 0)),
            pl.BlockSpec((256, 3 * rank), lambda i: (i, 0)),
            pl.BlockSpec((3 * rank, rhs), lambda i: (0, 0)),
            ANY,
        ],
        out_specs=pl.BlockSpec((256, rhs), lambda i: (i, 0)),
        out_shape=pltpu.VMEM((n, rhs), F32),
        compiler_params=grant(12),
        cost_estimate=pl.CostEstimate(flops=2_000_000_000, bytes_accessed=8_000_000, transcendentals=0),
    )(*in_hbm(ordered, leaves), et, fe, far)
    far = lax.all_to_all(far, ("zl", "x"), 0, 0, tiled=True)
    far = lax.all_gather(far.reshape(half, rhs), "c", axis=0, tiled=True)
    step = 256
    return pl.pallas_call(
        last_kernel,
        name="last",
        grid=(n // step,),
        in_specs=[
            pl.BlockSpec((2 * half, rhs), lambda i: (0, 0)),
            pl.BlockSpec((step, 2 * half), lambda i: (i, 0)),
            pl.BlockSpec((step, rhs), lambda i: (i, 0)),
        ],
        out_specs=pl.BlockSpec((step, rhs), lambda i: (i, 0)),
        out_shape=shape((n, rhs), BF16),
        scratch_shapes=[pltpu.VMEM((2 * half, rhs), BF16)],
        compiler_params=grant(8),
    )(far, *in_vmem(ut), base)


def solution(mesh):
    torus = Mesh(mesh.devices.reshape(4, 4, 4, 4, 2), AXES)
    placed = (P(AXES, None), P(AXES), P(AXES, None), P(None, None, AXES), P(None, None, AXES), P())
    return jax.shard_map(
        per_device, mesh=torus, in_specs=placed, out_specs=P(AXES, None), check_vma=False
    )
```

```python
import jax
import jax.numpy as jnp
from jax import lax
from jax.experimental import pallas as pl
from jax.experimental.pallas import tpu as pltpu
from jax.sharding import Mesh
from jax.sharding import PartitionSpec as P

AXES = ("y", "zh", "z1", "z0", "x", "c")
OUTER = ("z0", "x")
MIDDLE = ("y", "zh", "z1")
F32 = jnp.float32
BF16 = jnp.bfloat16
NN = (((1,), (0,)), ((), ()))
NT = (((1,), (1,)), ((), ()))


def dot(a, b, dims=NN):
    return lax.dot_general(a, b, dims, preferred_element_type=F32)


def one_hot_t(perm, first, count):
    n = perm.shape[1]
    j = lax.broadcasted_iota(jnp.int32, (count, n), 0) + first
    return jnp.where(j == perm, 1.0, 0.0).astype(BF16)


def coef_kernel(core, perm_hbm, v_hbm, s_hbm, mine_ref, send_ref, acc, perm_ref, v_ref, s_ref, perm_sem, v_sem, s_sem):
    n = s_ref.shape[0]
    levels, rank, _ = v_ref.shape
    step = 256
    perm_copy = pltpu.make_async_copy(perm_hbm, perm_ref, perm_sem)
    perm_copy.start()
    v_copy = pltpu.make_async_copy(v_hbm.at[0:levels], v_ref, v_sem)
    v_copy.start()
    s_copy = [
        pltpu.make_async_copy(s_hbm.at[j : j + step], s_ref.at[j : j + step], s_sem.at[j // step])
        for j in range(0, n, step)
    ]
    for copy in s_copy:
        copy.start()
    perm_copy.wait()
    perm = perm_ref[...] & (n - 1)
    hot = one_hot_t(perm, 0, step)
    v_copy.wait()
    v = v_ref[...].reshape(levels * rank, n)
    total = None
    for j in range(0, n, step):
        vp = dot(v, hot, NT).astype(BF16)
        if j + step < n:
            hot = one_hot_t(perm, j + step, step)
        s_copy[j // step].wait()
        part = dot(vp, s_ref[j : j + step, :])
        total = part if total is None else total + part
    half = 4 * rank
    me = core[0]
    mine = pl.ds(pl.multiple_of(me * half, half), half)
    theirs = pl.ds(pl.multiple_of((1 - me) * half, half), half)
    for d in range(acc.shape[0]):
        lanes = slice(d * 128, (d + 1) * 128)
        for level in range(8):
            acc[d, pl.ds(level, rank, stride=8), :] = total[level * rank : (level + 1) * rank, lanes]
        mine_ref[:, lanes] = acc[d, mine, :]
        send_ref[0:half, lanes] = acc[d, theirs, :]
    send_ref[half : half + rank, :] = total[8 * rank : 9 * rank]


def order_kernel(
    core, perm_hbm, s_hbm, v_hbm, pair_ref, _,
    ord_hbm, fe_ref, token_ref,
    perm_ref, s_ref, v_ref, p_ref, ord_ref, sems, ord_sems,
):
    n, _ = s_ref.shape
    rank = v_ref.shape[0]
    leaf = n // 2
    step = 256
    pairs = ((perm_hbm, perm_ref), (s_hbm, s_ref), (v_hbm.at[9], v_ref))
    copies = [pltpu.make_async_copy(a, b, sems.at[k]) for k, (a, b) in enumerate(pairs)]
    for copy in copies:
        copy.start()
    copies[0].wait()
    perm = perm_ref[...] & (n - 1)
    lane = lax.broadcasted_iota(jnp.int32, (128, 128), 1)
    for i in range(0, n, 128):
        column = jnp.broadcast_to(perm[:, i : i + 128], (128, 128)).T
        for j in range(0, n, 128):
            p_ref[i : i + 128, j : j + 128] = jnp.where(column == lane + j, 1.0, 0.0).astype(BF16)
    for copy in copies[1:]:
        copy.wait()

    def kept_copy(b):
        rows = pl.ds(pl.multiple_of(b * step, step), step)
        return pltpu.make_async_copy(ord_ref.at[rows], ord_hbm.at[rows], ord_sems.at[b])

    def order(b, _):
        rows = pl.ds(pl.multiple_of(b * step, step), step)
        ord_ref[rows, :] = dot(p_ref[rows, :], s_ref[...]).astype(BF16)
        kept_copy(b).start()
        return 0

    lax.fori_loop(0, n // step, order, 0)
    fe_ref[0:rank, :] = pair_ref[1 - core[0], 4 * rank :, :].astype(BF16)
    fe_ref[rank : 2 * rank, :] = dot(v_ref[:, leaf:], ord_ref[leaf:, :]).astype(BF16)
    fe_ref[2 * rank : 3 * rank, :] = dot(v_ref[:, :leaf], ord_ref[:leaf, :]).astype(BF16)
    token_ref[...] = jnp.zeros_like(token_ref)
    for b in range(n // step):
        kept_copy(b).wait()


def bases_kernel(
    ranks, perm_hbm, leaf_hbm, u_hbm, _,
    lp_hbm, ut_ref, et_ref, token_ref,
    perm_ref, leaf_ref, u_ref, pt_ref, uf_ref, us_ref, ue_ref, lp_ref, sems, lp_sems,
):
    n, leaf = leaf_ref.shape
    rank = u_ref.shape[1]
    step = 256
    pairs = ((perm_hbm, perm_ref), (leaf_hbm, leaf_ref), (u_hbm, u_ref))
    copies = [pltpu.make_async_copy(a, b, sems.at[k]) for k, (a, b) in enumerate(pairs)]
    for copy in copies:
        copy.start()
    copies[0].wait()
    perm = perm_ref[...] & (n - 1)
    for j in range(0, n, step):
        pt_ref[j : j + step, :] = one_hot_t(perm, j, step)
    for copy in copies[1:]:
        copy.wait()

    row = lax.broadcasted_iota(jnp.int32, (rank, n), 0)
    lane_n = lax.broadcasted_iota(jnp.int32, (rank, n), 1)
    for level in range(8):
        kept = jnp.where(row < ranks[level], u_ref[level].astype(F32), 0.0)
        for d in range(n // 128):
            uf_ref[d, pl.ds(level, rank, stride=8), :] = kept[:, d * 128 : (d + 1) * 128]
    for d in range(n // 128):
        us_ref[:, d * 128 : (d + 1) * 128] = uf_ref[d].astype(BF16)
    ue_ref[0:rank, :] = jnp.where(row < ranks[8], u_ref[8].astype(F32), 0.0).astype(BF16)
    last = jnp.where(row < ranks[9], u_ref[9].astype(F32), 0.0)
    ue_ref[rank : 2 * rank, :] = jnp.where(lane_n < leaf, last, 0.0).astype(BF16)
    ue_ref[2 * rank : 3 * rank, :] = jnp.where(lane_n < leaf, 0.0, last).astype(BF16)

    def kept_copy(b):
        rows = pl.ds(pl.multiple_of(b * step, step), step)
        return pltpu.make_async_copy(lp_ref.at[rows], lp_hbm.at[rows], lp_sems.at[b])

    def permute(b, _):
        rows = pl.ds(pl.multiple_of(b * step, step), step)
        for g in range(0, n, leaf):
            lp_ref[rows, g : g + leaf] = dot(pt_ref[rows, g : g + leaf], leaf_ref[g : g + leaf, :]).astype(BF16)
        kept_copy(b).start()
        ut_ref[rows, :] = dot(pt_ref[rows, :], us_ref[...], NT).astype(BF16)
        et_ref[rows, :] = dot(pt_ref[rows, :], ue_ref[...], NT).astype(BF16)
        return 0

    lax.fori_loop(0, n // step, permute, 0)
    token_ref[...] = jnp.zeros_like(token_ref)
    for b in range(n // step):
        kept_copy(b).wait()


def base_kernel(ord_ref, lp_ref, et_ref, fe_ref, _, base_ref):
    base_ref[...] = dot(lp_ref[...], ord_ref[...]) + dot(et_ref[...], fe_ref[...])


def level_at(apart):
    for bit, row in ((16, 0), (8, 1), (4, 2), (2, 3)):
        if apart & bit:
            return row
    return 4


def middle_kernel(me, got_ref, _, out_ref, fine_ref):
    rows = got_ref.shape[1]
    level = lax.broadcasted_iota(jnp.int32, got_ref.shape[1:], 0) & 7
    got = lambda z, x: got_ref[z * 4 + x]
    sums = [(got(z, 0) + got(z, 1)) + (got(z, 2) + got(z, 3)) for z in range(2)]
    total = sums[0] + sums[1]
    for z in range(2):
        for x in range(4):
            high = jnp.where(level == 7, got(z, x ^ 1), got(z, x ^ 2) + got(z, x ^ 3))
            fine_ref[z * 4 + x] = jnp.where(level >= 6, high, sums[z ^ 1])
    for row in range(5):
        sent = jnp.concatenate([total[r + row : r + row + 1] for r in range(0, rows, 8)], axis=0)
        for apart in range(out_ref.shape[0]):
            if level_at(apart) == row:
                out_ref[me[0] ^ apart] = sent


def far_kernel(me, got_ref, fine_ref, _, out_ref, acc):
    rows = acc.shape[0]
    acc[...] = jnp.zeros_like(acc)
    for row in range(5):
        parts = [got_ref[me[0] ^ k] for k in range(1, got_ref.shape[0]) if level_at(k) == row]
        while len(parts) > 1:
            parts = [sum(parts[k : k + 2]) for k in range(0, len(parts), 2)]
        for j in range(rows // 8):
            acc[j * 8 + row : j * 8 + row + 1, :] = parts[0][j : j + 1]
    level = lax.broadcasted_iota(jnp.int32, acc.shape, 0) & 7
    far = acc[...]
    for p in range(out_ref.shape[0]):
        out_ref[p] = jnp.where(level < 5, far, fine_ref[p])


def last_kernel(far_ref, ut_ref, base_ref, out_ref, far16):
    @pl.when(pl.program_id(0) == 0)
    def _():
        far16[...] = far_ref[...].astype(BF16)

    out_ref[...] = (base_ref[...] + dot(ut_ref[...], far16[...])).astype(BF16)


SMEM = pl.BlockSpec(memory_space=pltpu.SMEM)
VMEM = pl.BlockSpec(memory_space=pltpu.VMEM)
ANY = pl.BlockSpec(memory_space=pl.ANY)
HBM = pl.BlockSpec(memory_space=pltpu.HBM)


def grant(mib):
    return pltpu.CompilerParams(vmem_limit_bytes=mib << 20)


def in_hbm(*arrays):
    return [pltpu.with_memory_space_constraint(a, pltpu.HBM) for a in arrays]


def in_vmem(*arrays):
    return [pltpu.with_memory_space_constraint(a, pltpu.VMEM) for a in arrays]


def shape(dims, dtype=F32):
    return jax.ShapeDtypeStruct(dims, dtype)


def per_device(sources, tree_perm, leaf_blocks, u_factors, v_factors, level_ranks):
    n, rhs = sources.shape
    rank = u_factors.shape[1]
    half = 4 * rank
    core = lax.axis_index("c").reshape(1)
    me = lax.axis_index(MIDDLE).reshape(1)
    perm = tree_perm.reshape(1, n)
    mine, send = pl.pallas_call(
        coef_kernel,
        name="coef",
        in_specs=[SMEM, HBM, HBM, HBM],
        out_specs=[VMEM, VMEM],
        out_shape=[shape((half, rhs)), shape((half + rank, rhs))],
        scratch_shapes=[
            pltpu.VMEM((rhs // 128, 2 * half, 128), F32),
            pltpu.VMEM((1, n), jnp.int32),
            pltpu.VMEM((9, rank, n), BF16),
            pltpu.VMEM((n, rhs), BF16),
            pltpu.SemaphoreType.DMA,
            pltpu.SemaphoreType.DMA,
            pltpu.SemaphoreType.DMA((n // 256,)),
        ],
        compiler_params=grant(14),
    )(core, *in_hbm(perm, v_factors, sources))
    pair = lax.all_gather(send, "c")
    other = lax.dynamic_index_in_dim(pair, 1 - core[0], 0, keepdims=False)
    partial = (mine + other[:half]).reshape(8, 16, rhs)
    ordered, fe, token = pl.pallas_call(
        order_kernel,
        name="order",
        in_specs=[SMEM, HBM, HBM, HBM, VMEM, ANY],
        out_specs=[HBM, VMEM, VMEM],
        out_shape=[pltpu.HBM((n, rhs), BF16), pltpu.VMEM((3 * rank, rhs), BF16), shape((8, 128))],
        scratch_shapes=[
            pltpu.VMEM((1, n), jnp.int32),
            pltpu.VMEM((n, rhs), BF16),
            pltpu.VMEM((rank, n), BF16),
            pltpu.VMEM((n, n), BF16),
            pltpu.VMEM((n, rhs), BF16),
            pltpu.SemaphoreType.DMA((3,)),
            pltpu.SemaphoreType.DMA((n // 256,)),
        ],
        compiler_params=grant(16),
        cost_estimate=pl.CostEstimate(flops=2_000_000_000, bytes_accessed=4_000_000, transcendentals=0),
    )(core, *in_hbm(perm, sources, v_factors), *in_vmem(pair), partial)
    got = lax.all_to_all(partial, OUTER, 0, 0, tiled=True)
    rows, fine = pl.pallas_call(
        middle_kernel,
        name="middle",
        in_specs=[SMEM, VMEM, ANY],
        out_specs=[VMEM, VMEM],
        out_shape=[shape((32, 2, rhs)), shape((8, 16, rhs))],
        compiler_params=grant(4),
    )(me, got, token)
    leaves, ut, et, token = pl.pallas_call(
        bases_kernel,
        name="bases",
        in_specs=[SMEM, HBM, HBM, HBM, ANY],
        out_specs=[HBM, VMEM, VMEM, VMEM],
        out_shape=[
            pltpu.HBM((n, n), BF16),
            pltpu.VMEM((n, 2 * half), BF16),
            pltpu.VMEM((n, 3 * rank), BF16),
            shape((8, 128)),
        ],
        scratch_shapes=[
            pltpu.VMEM((1, n), jnp.int32),
            pltpu.VMEM(leaf_blocks.shape, BF16),
            pltpu.VMEM(u_factors.shape, BF16),
            pltpu.VMEM((n, n), BF16),
            pltpu.VMEM((n // 128, 2 * half, 128), F32),
            pltpu.VMEM((2 * half, n), BF16),
            pltpu.VMEM((3 * rank, n), BF16),
            pltpu.VMEM((n, n), BF16),
            pltpu.SemaphoreType.DMA((3,)),
            pltpu.SemaphoreType.DMA((n // 256,)),
        ],
        compiler_params=grant(20),
        cost_estimate=pl.CostEstimate(flops=2_000_000_000, bytes_accessed=4_000_000, transcendentals=0),
    )(level_ranks, *in_hbm(perm, leaf_blocks, u_factors), fine)
    rows = lax.all_to_all(rows, MIDDLE, 0, 0, tiled=True)
    far = pl.pallas_call(
        far_kernel,
        name="far",
        in_specs=[SMEM, VMEM, VMEM, ANY],
        out_specs=VMEM,
        out_shape=shape((8, 16, rhs)),
        scratch_shapes=[pltpu.VMEM((16, rhs), F32)],
        compiler_params=grant(4),
    )(me, rows, fine, token)
    base = pl.pallas_call(
        base_kernel,
        name="base",
        grid=(n // 256,),
        in_specs=[
            pl.BlockSpec((n, rhs), lambda i: (0, 0)),
            pl.BlockSpec((256, n), lambda i: (i, 0)),
            pl.BlockSpec((256, 3 * rank), lambda i: (i, 0)),
            pl.BlockSpec((3 * rank, rhs), lambda i: (0, 0)),
            ANY,
        ],
        out_specs=pl.BlockSpec((256, rhs), lambda i: (i, 0)),
        out_shape=pltpu.VMEM((n, rhs), F32),
        compiler_params=grant(12),
        cost_estimate=pl.CostEstimate(flops=2_000_000_000, bytes_accessed=8_000_000, transcendentals=0),
    )(*in_hbm(ordered, leaves), et, fe, far)
    far = lax.all_to_all(far, OUTER, 0, 0, tiled=True)
    far = lax.all_gather(far.reshape(half, rhs), "c", axis=0, tiled=True)
    step = 256
    return pl.pallas_call(
        last_kernel,
        name="last",
        grid=(n // step,),
        in_specs=[
            pl.BlockSpec((2 * half, rhs), lambda i: (0, 0)),
            pl.BlockSpec((step, 2 * half), lambda i: (i, 0)),
            pl.BlockSpec((step, rhs), lambda i: (i, 0)),
        ],
        out_specs=pl.BlockSpec((step, rhs), lambda i: (i, 0)),
        out_shape=shape((n, rhs), BF16),
        scratch_shapes=[pltpu.VMEM((2 * half, rhs), BF16)],
        compiler_params=grant(8),
    )(far, *in_vmem(ut), base)


def solution(mesh):
    torus = Mesh(mesh.devices.reshape(4, 4, 2, 2, 4, 2), AXES)
    placed = (P(AXES, None), P(AXES), P(AXES, None), P(None, None, AXES), P(None, None, AXES), P())
    return jax.shard_map(
        per_device, mesh=torus, in_specs=placed, out_specs=P(AXES, None), check_vma=False
    )
```

```python
import jax
import jax.numpy as jnp
from jax import lax
from jax.experimental import pallas as pl
from jax.experimental.pallas import tpu as pltpu
from jax.sharding import Mesh
from jax.sharding import PartitionSpec as P

AXES = ("y", "zh", "z1", "z0", "x", "c")
OUTER = ("z0", "x")
MIDDLE = ("y", "zh", "z1")
F32 = jnp.float32
BF16 = jnp.bfloat16
NN = (((1,), (0,)), ((), ()))
NT = (((1,), (1,)), ((), ()))


def dot(a, b, dims=NN):
    return lax.dot_general(a, b, dims, preferred_element_type=F32)


def one_hot_t(perm, first, count):
    n = perm.shape[1]
    j = lax.broadcasted_iota(jnp.int32, (count, n), 0) + first
    return jnp.where(j == perm, 1.0, 0.0).astype(BF16)


def coef_kernel(core, perm_hbm, v_hbm, s_hbm, mine_ref, send_ref, acc, perm_ref, v_ref, s_ref, perm_sem, v_sem, s_sem):
    n = s_ref.shape[0]
    levels, rank, _ = v_ref.shape
    step = 256
    perm_copy = pltpu.make_async_copy(perm_hbm, perm_ref, perm_sem)
    perm_copy.start()
    v_copy = pltpu.make_async_copy(v_hbm.at[0:levels], v_ref, v_sem)
    v_copy.start()

    def s_copy(k):
        rows = pl.ds(pl.multiple_of(k * step, step), step)
        return pltpu.make_async_copy(s_hbm.at[rows], s_ref.at[rows], s_sem.at[k])

    def start(k, _):
        s_copy(k).start()
        return 0

    lax.fori_loop(0, n // step, start, 0)
    perm_copy.wait()
    perm = perm_ref[...] & (n - 1)
    hot = one_hot_t(perm, 0, step)
    v_copy.wait()
    v = v_ref[...].reshape(levels * rank, n)
    total = None
    for j in range(0, n, step):
        vp = dot(v, hot, NT).astype(BF16)
        if j + step < n:
            hot = one_hot_t(perm, j + step, step)
        s_copy(j // step).wait()
        part = dot(vp, s_ref[j : j + step, :])
        total = part if total is None else total + part
    half = 4 * rank
    me = core[0]
    mine = pl.ds(pl.multiple_of(me * half, half), half)
    theirs = pl.ds(pl.multiple_of((1 - me) * half, half), half)
    for d in range(acc.shape[0]):
        lanes = slice(d * 128, (d + 1) * 128)
        for level in range(8):
            acc[d, pl.ds(level, rank, stride=8), :] = total[level * rank : (level + 1) * rank, lanes]
        mine_ref[:, lanes] = acc[d, mine, :]
        send_ref[0:half, lanes] = acc[d, theirs, :]
    send_ref[half : half + rank, :] = total[8 * rank : 9 * rank]


def order_kernel(
    core, perm_hbm, s_hbm, v_hbm, pair_ref, _,
    ord_hbm, fe_ref, token_ref,
    perm_ref, s_ref, v_ref, p_ref, ord_ref, sems, ord_sems,
):
    n, _ = s_ref.shape
    rank = v_ref.shape[0]
    leaf = n // 2
    step = 256
    pairs = ((perm_hbm, perm_ref), (s_hbm, s_ref), (v_hbm.at[9], v_ref))
    copies = [pltpu.make_async_copy(a, b, sems.at[k]) for k, (a, b) in enumerate(pairs)]
    for copy in copies:
        copy.start()
    copies[0].wait()
    perm = perm_ref[...] & (n - 1)
    lane = lax.broadcasted_iota(jnp.int32, (128, 128), 1)

    def kept_copy(b):
        rows = slice(b * step, (b + 1) * step)
        return pltpu.make_async_copy(ord_ref.at[rows], ord_hbm.at[rows], ord_sems.at[b])

    for b in range(n // step):
        rows = slice(b * step, (b + 1) * step)
        for i in range(b * step, (b + 1) * step, 128):
            column = jnp.broadcast_to(perm[:, i : i + 128], (128, 128)).T
            for j in range(0, n, 128):
                p_ref[i : i + 128, j : j + 128] = jnp.where(column == lane + j, 1.0, 0.0).astype(BF16)
        if b == 0:
            copies[1].wait()
        ord_ref[rows, :] = dot(p_ref[rows, :], s_ref[...]).astype(BF16)
        kept_copy(b).start()
    copies[2].wait()
    fe_ref[0:rank, :] = pair_ref[1 - core[0], 4 * rank :, :].astype(BF16)
    fe_ref[rank : 2 * rank, :] = dot(v_ref[:, leaf:], ord_ref[leaf:, :]).astype(BF16)
    fe_ref[2 * rank : 3 * rank, :] = dot(v_ref[:, :leaf], ord_ref[:leaf, :]).astype(BF16)
    token_ref[...] = jnp.zeros_like(token_ref)
    for b in range(n // step):
        kept_copy(b).wait()


def bases_kernel(
    ranks, perm_hbm, leaf_hbm, u_hbm, _,
    lp_hbm, ut_ref, et_ref, token_ref,
    perm_ref, leaf_ref, u_ref, pt_ref, uf_ref, us_ref, ue_ref, lp_ref, sems, lp_sems,
):
    n, leaf = leaf_ref.shape
    rank = u_ref.shape[1]
    step = 256
    pairs = ((perm_hbm, perm_ref), (leaf_hbm, leaf_ref), (u_hbm, u_ref))
    copies = [pltpu.make_async_copy(a, b, sems.at[k]) for k, (a, b) in enumerate(pairs)]
    for copy in copies:
        copy.start()
    copies[0].wait()
    perm = perm_ref[...] & (n - 1)
    for j in range(0, n, step):
        pt_ref[j : j + step, :] = one_hot_t(perm, j, step)
    for copy in copies[1:]:
        copy.wait()

    row = lax.broadcasted_iota(jnp.int32, (rank, n), 0)
    lane_n = lax.broadcasted_iota(jnp.int32, (rank, n), 1)
    for level in range(8):
        kept = jnp.where(row < ranks[level], u_ref[level].astype(F32), 0.0)
        for d in range(n // 128):
            uf_ref[d, pl.ds(level, rank, stride=8), :] = kept[:, d * 128 : (d + 1) * 128]
    for d in range(n // 128):
        us_ref[:, d * 128 : (d + 1) * 128] = uf_ref[d].astype(BF16)
    ue_ref[0:rank, :] = jnp.where(row < ranks[8], u_ref[8].astype(F32), 0.0).astype(BF16)
    last = jnp.where(row < ranks[9], u_ref[9].astype(F32), 0.0)
    ue_ref[rank : 2 * rank, :] = jnp.where(lane_n < leaf, last, 0.0).astype(BF16)
    ue_ref[2 * rank : 3 * rank, :] = jnp.where(lane_n < leaf, 0.0, last).astype(BF16)

    def kept_copy(b):
        rows = pl.ds(pl.multiple_of(b * step, step), step)
        return pltpu.make_async_copy(lp_ref.at[rows], lp_hbm.at[rows], lp_sems.at[b])

    def permute(b, _):
        rows = pl.ds(pl.multiple_of(b * step, step), step)
        for g in range(0, n, leaf):
            lp_ref[rows, g : g + leaf] = dot(pt_ref[rows, g : g + leaf], leaf_ref[g : g + leaf, :]).astype(BF16)
        kept_copy(b).start()
        ut_ref[rows, :] = dot(pt_ref[rows, :], us_ref[...], NT).astype(BF16)
        et_ref[rows, :] = dot(pt_ref[rows, :], ue_ref[...], NT).astype(BF16)
        return 0

    lax.fori_loop(0, n // step, permute, 0)
    token_ref[...] = jnp.zeros_like(token_ref)
    for b in range(n // step):
        kept_copy(b).wait()


def base_kernel(ord_hbm, lp_hbm, et_ref, fe_ref, _, base_ref, ord_ref, lp_ref, ord_sem, lp_sems):
    n, step = lp_ref.shape[0], 256
    ord_copy = pltpu.make_async_copy(ord_hbm, ord_ref, ord_sem)
    ord_copy.start()

    def block(b):
        return pl.ds(pl.multiple_of(b * step, step), step)

    def lp_copy(b):
        return pltpu.make_async_copy(lp_hbm.at[block(b)], lp_ref.at[block(b)], lp_sems.at[b])

    def first(b, _):
        lp_copy(b).start()
        base_ref[block(b), :] = dot(et_ref[block(b), :], fe_ref[...])
        return 0

    lax.fori_loop(0, n // step, first, 0)
    ord_copy.wait()

    def second(b, _):
        lp_copy(b).wait()
        base_ref[block(b), :] += dot(lp_ref[block(b), :], ord_ref[...])
        return 0

    lax.fori_loop(0, n // step, second, 0)


def level_at(apart):
    for bit, row in ((16, 0), (8, 1), (4, 2), (2, 3)):
        if apart & bit:
            return row
    return 4


def middle_kernel(me, got_ref, _, out_ref, fine_ref):
    rows = got_ref.shape[1]
    level = lax.broadcasted_iota(jnp.int32, got_ref.shape[1:], 0) & 7
    got = lambda z, x: got_ref[z * 4 + x]
    sums = [(got(z, 0) + got(z, 1)) + (got(z, 2) + got(z, 3)) for z in range(2)]
    total = sums[0] + sums[1]
    for z in range(2):
        for x in range(4):
            high = jnp.where(level == 7, got(z, x ^ 1), got(z, x ^ 2) + got(z, x ^ 3))
            fine_ref[z * 4 + x] = jnp.where(level >= 6, high, sums[z ^ 1])
    for row in range(5):
        sent = jnp.concatenate([total[r + row : r + row + 1] for r in range(0, rows, 8)], axis=0)
        for apart in range(out_ref.shape[0]):
            if level_at(apart) == row:
                out_ref[me[0] ^ apart] = sent


def far_kernel(me, got_ref, fine_ref, _, out_ref, acc):
    rows = acc.shape[0]
    acc[...] = jnp.zeros_like(acc)
    for row in range(5):
        parts = [got_ref[me[0] ^ k] for k in range(1, got_ref.shape[0]) if level_at(k) == row]
        while len(parts) > 1:
            parts = [sum(parts[k : k + 2]) for k in range(0, len(parts), 2)]
        for j in range(rows // 8):
            acc[j * 8 + row : j * 8 + row + 1, :] = parts[0][j : j + 1]
    level = lax.broadcasted_iota(jnp.int32, acc.shape, 0) & 7
    far = acc[...]
    for p in range(out_ref.shape[0]):
        out_ref[p] = jnp.where(level < 5, far, fine_ref[p])


def last_kernel(far_ref, ut_ref, base_ref, out_hbm, far16, out_ref, sems):
    n, step = base_ref.shape[0], 256
    far16[...] = far_ref[...].astype(BF16)

    def out_copy(b):
        rows = pl.ds(pl.multiple_of(b * step, step), step)
        return pltpu.make_async_copy(out_ref.at[rows], out_hbm.at[rows], sems.at[b])

    def apply(b, _):
        rows = pl.ds(pl.multiple_of(b * step, step), step)
        out_ref[rows, :] = (base_ref[rows, :] + dot(ut_ref[rows, :], far16[...])).astype(BF16)
        out_copy(b).start()
        return 0

    lax.fori_loop(0, n // step, apply, 0)
    for b in range(n // step):
        out_copy(b).wait()


SMEM = pl.BlockSpec(memory_space=pltpu.SMEM)
VMEM = pl.BlockSpec(memory_space=pltpu.VMEM)
ANY = pl.BlockSpec(memory_space=pl.ANY)
HBM = pl.BlockSpec(memory_space=pltpu.HBM)


def grant(mib):
    return pltpu.CompilerParams(vmem_limit_bytes=mib << 20)


def in_hbm(*arrays):
    return [pltpu.with_memory_space_constraint(a, pltpu.HBM) for a in arrays]


def in_vmem(*arrays):
    return [pltpu.with_memory_space_constraint(a, pltpu.VMEM) for a in arrays]


def shape(dims, dtype=F32):
    return jax.ShapeDtypeStruct(dims, dtype)


def per_device(sources, tree_perm, leaf_blocks, u_factors, v_factors, level_ranks):
    n, rhs = sources.shape
    rank = u_factors.shape[1]
    half = 4 * rank
    core = lax.axis_index("c").reshape(1)
    me = lax.axis_index(MIDDLE).reshape(1)
    perm = tree_perm.reshape(1, n)
    mine, send = pl.pallas_call(
        coef_kernel,
        name="coef",
        in_specs=[SMEM, HBM, HBM, HBM],
        out_specs=[VMEM, VMEM],
        out_shape=[shape((half, rhs)), shape((half + rank, rhs))],
        scratch_shapes=[
            pltpu.VMEM((rhs // 128, 2 * half, 128), F32),
            pltpu.VMEM((1, n), jnp.int32),
            pltpu.VMEM((9, rank, n), BF16),
            pltpu.VMEM((n, rhs), BF16),
            pltpu.SemaphoreType.DMA,
            pltpu.SemaphoreType.DMA,
            pltpu.SemaphoreType.DMA((n // 256,)),
        ],
        compiler_params=grant(14),
    )(core, *in_hbm(perm, v_factors, sources))
    pair = lax.all_gather(send, "c")
    other = lax.dynamic_index_in_dim(pair, 1 - core[0], 0, keepdims=False)
    partial = (mine + other[:half]).reshape(8, 16, rhs)
    ordered, fe, token = pl.pallas_call(
        order_kernel,
        name="order",
        in_specs=[SMEM, HBM, HBM, HBM, VMEM, ANY],
        out_specs=[HBM, VMEM, VMEM],
        out_shape=[pltpu.HBM((n, rhs), BF16), pltpu.VMEM((3 * rank, rhs), BF16), shape((8, 128))],
        scratch_shapes=[
            pltpu.VMEM((1, n), jnp.int32),
            pltpu.VMEM((n, rhs), BF16),
            pltpu.VMEM((rank, n), BF16),
            pltpu.VMEM((n, n), BF16),
            pltpu.VMEM((n, rhs), BF16),
            pltpu.SemaphoreType.DMA((3,)),
            pltpu.SemaphoreType.DMA((n // 256,)),
        ],
        compiler_params=grant(16),
        cost_estimate=pl.CostEstimate(flops=2_000_000_000, bytes_accessed=4_000_000, transcendentals=0),
    )(core, *in_hbm(perm, sources, v_factors), *in_vmem(pair), partial)
    got = lax.all_to_all(partial, OUTER, 0, 0, tiled=True)
    rows, fine = pl.pallas_call(
        middle_kernel,
        name="middle",
        in_specs=[SMEM, VMEM, ANY],
        out_specs=[VMEM, VMEM],
        out_shape=[shape((32, 2, rhs)), shape((8, 16, rhs))],
        compiler_params=grant(4),
    )(me, got, token)
    leaves, ut, et, token = pl.pallas_call(
        bases_kernel,
        name="bases",
        in_specs=[SMEM, HBM, HBM, HBM, ANY],
        out_specs=[HBM, VMEM, VMEM, VMEM],
        out_shape=[
            pltpu.HBM((n, n), BF16),
            pltpu.VMEM((n, 2 * half), BF16),
            pltpu.VMEM((n, 3 * rank), BF16),
            shape((8, 128)),
        ],
        scratch_shapes=[
            pltpu.VMEM((1, n), jnp.int32),
            pltpu.VMEM(leaf_blocks.shape, BF16),
            pltpu.VMEM(u_factors.shape, BF16),
            pltpu.VMEM((n, n), BF16),
            pltpu.VMEM((n // 128, 2 * half, 128), F32),
            pltpu.VMEM((2 * half, n), BF16),
            pltpu.VMEM((3 * rank, n), BF16),
            pltpu.VMEM((n, n), BF16),
            pltpu.SemaphoreType.DMA((3,)),
            pltpu.SemaphoreType.DMA((n // 256,)),
        ],
        compiler_params=grant(20),
        cost_estimate=pl.CostEstimate(flops=2_000_000_000, bytes_accessed=4_000_000, transcendentals=0),
    )(level_ranks, *in_hbm(perm, leaf_blocks, u_factors), fine)
    rows = lax.all_to_all(rows, MIDDLE, 0, 0, tiled=True)
    far = pl.pallas_call(
        far_kernel,
        name="far",
        in_specs=[SMEM, VMEM, VMEM, ANY],
        out_specs=VMEM,
        out_shape=shape((8, 16, rhs)),
        scratch_shapes=[pltpu.VMEM((16, rhs), F32)],
        compiler_params=grant(4),
    )(me, rows, fine, token)
    base = pl.pallas_call(
        base_kernel,
        name="base",
        in_specs=[HBM, HBM, VMEM, VMEM, ANY],
        out_specs=VMEM,
        out_shape=pltpu.VMEM((n, rhs), F32),
        scratch_shapes=[
            pltpu.VMEM((n, rhs), BF16),
            pltpu.VMEM((n, n), BF16),
            pltpu.SemaphoreType.DMA,
            pltpu.SemaphoreType.DMA((n // 256,)),
        ],
        compiler_params=grant(12),
        cost_estimate=pl.CostEstimate(flops=2_000_000_000, bytes_accessed=8_000_000, transcendentals=0),
    )(*in_hbm(ordered, leaves), *in_vmem(et, fe), far)
    far = lax.all_to_all(far, OUTER, 0, 0, tiled=True)
    far = lax.all_gather(far.reshape(half, rhs), "c", axis=0, tiled=True)
    return pl.pallas_call(
        last_kernel,
        name="last",
        in_specs=[VMEM] * 3,
        out_specs=HBM,
        out_shape=pltpu.HBM((n, rhs), BF16),
        scratch_shapes=[
            pltpu.VMEM((2 * half, rhs), BF16),
            pltpu.VMEM((n, rhs), BF16),
            pltpu.SemaphoreType.DMA((n // 256,)),
        ],
        compiler_params=grant(8),
    )(*in_vmem(far, ut, base))


def solution(mesh):
    torus = Mesh(mesh.devices.reshape(4, 4, 2, 2, 4, 2), AXES)
    placed = (P(AXES, None), P(AXES), P(AXES, None), P(None, None, AXES), P(None, None, AXES), P())
    return jax.shard_map(
        per_device, mesh=torus, in_specs=placed, out_specs=P(AXES, None), check_vma=False
    )
```

```python
import jax
import jax.numpy as jnp
from jax import lax
from jax.experimental import pallas as pl
from jax.experimental.pallas import tpu as pltpu
from jax.sharding import Mesh
from jax.sharding import PartitionSpec as P

AXES = ("y", "zh", "z1", "z0", "x", "c")
OUTER = ("z0", "x")
MIDDLE = ("y", "zh", "z1")
F32 = jnp.float32
BF16 = jnp.bfloat16
NN = (((1,), (0,)), ((), ()))
NT = (((1,), (1,)), ((), ()))


def dot(a, b, dims=NN):
    return lax.dot_general(a, b, dims, preferred_element_type=F32)


def one_hot_t(perm, first, count):
    n = perm.shape[1]
    j = lax.broadcasted_iota(jnp.int32, (count, n), 0) + first
    return jnp.where(j == perm, 1.0, 0.0).astype(BF16)


def coef_kernel(core, perm_hbm, v_hbm, s_hbm, mine_ref, send_ref, acc, perm_ref, v_ref, s_ref, perm_sem, v_sem, s_sem):
    n = s_ref.shape[0]
    levels, rank, _ = v_ref.shape
    step = 256
    perm_copy = pltpu.make_async_copy(perm_hbm, perm_ref, perm_sem)
    perm_copy.start()
    v_copy = pltpu.make_async_copy(v_hbm.at[0:levels], v_ref, v_sem)
    v_copy.start()

    def s_copy(k):
        rows = pl.ds(pl.multiple_of(k * step, step), step)
        return pltpu.make_async_copy(s_hbm.at[rows], s_ref.at[rows], s_sem.at[k])

    def start(k, _):
        s_copy(k).start()
        return 0

    lax.fori_loop(0, n // step, start, 0)
    perm_copy.wait()
    perm = perm_ref[...] & (n - 1)
    v_copy.wait()
    v = v_ref[...].reshape(levels * rank, n)
    vp = [dot(v, one_hot_t(perm, j, step), NT).astype(BF16) for j in range(0, n, step)]
    for k in range(n // step):
        s_copy(k).wait()
    total = dot(jnp.concatenate(vp, axis=1), s_ref[...])
    half = 4 * rank
    me = core[0]
    mine = pl.ds(pl.multiple_of(me * half, half), half)
    theirs = pl.ds(pl.multiple_of((1 - me) * half, half), half)
    for d in range(acc.shape[0]):
        lanes = slice(d * 128, (d + 1) * 128)
        for level in range(8):
            acc[d, pl.ds(level, rank, stride=8), :] = total[level * rank : (level + 1) * rank, lanes]
        mine_ref[:, lanes] = acc[d, mine, :]
        send_ref[0:half, lanes] = acc[d, theirs, :]
    send_ref[half : half + rank, :] = total[8 * rank : 9 * rank]


def add_kernel(core, _, mine_ref, pair_ref, out_ref):
    half = mine_ref.shape[0]
    out_ref[...] = mine_ref[...] + pair_ref[1 - core[0], 0:half, :]


def local_kernel(
    ranks, core, perm_hbm, s_hbm, leaf_hbm, u_hbm, v_hbm, pair_ref, _,
    top_ref, low_hbm, ut_ref, token_ref,
    perm_ref, s_ref, leaf_ref, u_ref, v_ref, ord_ref, uf_ref, us_ref, ue_ref, fe_ref, low_ref, sems, s_sem, leaf_sem, low_sem,
):
    n, leaf = leaf_ref.shape
    rank = v_ref.shape[0]
    step = 256
    pairs = ((perm_hbm, perm_ref), (u_hbm, u_ref), (v_hbm.at[9], v_ref))
    copies = [pltpu.make_async_copy(a, b, sems.at[k]) for k, (a, b) in enumerate(pairs)]
    for copy in copies:
        copy.start()

    def tall_copies(k):
        rows = pl.ds(pl.multiple_of(k * step, step), step)
        return (
            pltpu.make_async_copy(s_hbm.at[rows], s_ref.at[rows], s_sem.at[k]),
            pltpu.make_async_copy(leaf_hbm.at[rows], leaf_ref.at[rows], leaf_sem.at[k]),
        )

    def start(k, _):
        for copy in tall_copies(k):
            copy.start()
        return 0

    lax.fori_loop(0, n // step, start, 0)
    copies[0].wait()
    perm = perm_ref[...] & (n - 1)
    copies[1].wait()
    row = lax.broadcasted_iota(jnp.int32, (rank, n), 0)
    lane_n = lax.broadcasted_iota(jnp.int32, (rank, n), 1)
    for level in range(8):
        kept = jnp.where(row < ranks[level], u_ref[level].astype(F32), 0.0)
        for d in range(n // 128):
            uf_ref[d, pl.ds(level, rank, stride=8), :] = kept[:, d * 128 : (d + 1) * 128]
    for d in range(n // 128):
        us_ref[:, d * 128 : (d + 1) * 128] = uf_ref[d].astype(BF16)
    ue_ref[0:rank, :] = jnp.where(row < ranks[8], u_ref[8].astype(F32), 0.0).astype(BF16)
    last = jnp.where(row < ranks[9], u_ref[9].astype(F32), 0.0)
    ue_ref[rank : 2 * rank, :] = jnp.where(lane_n < leaf, last, 0.0).astype(BF16)
    ue_ref[2 * rank : 3 * rank, :] = jnp.where(lane_n < leaf, 0.0, last).astype(BF16)

    copies[2].wait()
    for k in range(n // step):
        for copy in tall_copies(k):
            copy.wait()
    lane = lax.broadcasted_iota(jnp.int32, (128, 128), 1)
    for i in range(0, n, step):
        hot = []
        for h in range(i, i + step, 128):
            column = jnp.broadcast_to(perm[:, h : h + 128], (128, 128)).T
            hot.append(
                jnp.concatenate(
                    [jnp.where(column == lane + j, 1.0, 0.0).astype(BF16) for j in range(0, n, 128)], axis=1
                )
            )
        ord_ref[i : i + step, :] = dot(jnp.concatenate(hot, axis=0), s_ref[...]).astype(BF16)
    fe_ref[0:rank, :] = pair_ref[1 - core[0], 4 * rank :, :].astype(BF16)
    fe_ref[rank : 2 * rank, :] = dot(v_ref[:, leaf:], ord_ref[leaf:, :]).astype(BF16)
    fe_ref[2 * rank : 3 * rank, :] = dot(v_ref[:, :leaf], ord_ref[:leaf, :]).astype(BF16)
    top = top_ref.shape[0]
    kept = []
    for j in [*range(top, n, step), *range(0, top, step)]:
        rows = slice(j, j + step)
        hot = one_hot_t(perm, j, step)
        leaves = [dot(hot[:, g : g + leaf], leaf_ref[g : g + leaf, :]).astype(BF16) for g in range(0, n, leaf)]
        ut_ref[rows, :] = dot(hot, us_ref[...], NT).astype(BF16)
        et = dot(hot, ue_ref[...], NT).astype(BF16)
        base = dot(jnp.concatenate(leaves, axis=1), ord_ref[...]) + dot(et, fe_ref[...])
        if j < top:
            top_ref[rows, :] = base
        else:
            part = slice(j - top, j - top + step)
            low_ref[part, :] = base
            kept.append(pltpu.make_async_copy(low_ref.at[part], low_hbm.at[part], low_sem.at[len(kept)]))
            kept[-1].start()
    token_ref[...] = jnp.zeros_like(token_ref)
    for copy in kept:
        copy.wait()


def level_at(apart):
    for bit, row in ((16, 0), (8, 1), (4, 2), (2, 3)):
        if apart & bit:
            return row
    return 4


def middle_kernel(me, got_ref, out_ref, fine_ref, token_ref):
    token_ref[...] = jnp.zeros_like(token_ref)
    rows = got_ref.shape[1]
    got = lambda z, x: got_ref[z * 4 + x]
    sums = [(got(z, 0) + got(z, 1)) + (got(z, 2) + got(z, 3)) for z in range(2)]
    total = sums[0] + sums[1]
    for z in range(2):
        for x in range(4):
            for j in range(rows // 8):
                at = lambda a, row: a[j * 8 + row : j * 8 + row + 1]
                fine_ref[z * 4 + x, j * 4 : j * 4 + 1, :] = at(sums[z ^ 1], 5)
                fine_ref[z * 4 + x, j * 4 + 1 : j * 4 + 2, :] = at(got(z, x ^ 2), 6) + at(got(z, x ^ 3), 6)
                fine_ref[z * 4 + x, j * 4 + 2 : j * 4 + 3, :] = at(got(z, x ^ 1), 7)
    for row in range(5):
        sent = jnp.concatenate([total[r + row : r + row + 1] for r in range(0, rows, 8)], axis=0)
        for apart in range(out_ref.shape[0]):
            if level_at(apart) == row:
                out_ref[me[0] ^ apart] = sent


def far_kernel(me, got_ref, fine_ref, _, out_ref, acc):
    rows = acc.shape[0]
    acc[...] = jnp.zeros_like(acc)
    for row in range(5):
        parts = [got_ref[me[0] ^ k] for k in range(1, got_ref.shape[0]) if level_at(k) == row]
        while len(parts) > 1:
            parts = [sum(parts[k : k + 2]) for k in range(0, len(parts), 2)]
        for j in range(rows // 8):
            acc[j * 8 + row : j * 8 + row + 1, :] = parts[0][j : j + 1]
    far = acc[...]
    for p in range(out_ref.shape[0]):
        out_ref[p] = far
        for j in range(rows // 8):
            out_ref[p, j * 8 + 5 : j * 8 + 8, :] = fine_ref[p, j * 4 : j * 4 + 3, :]


def last_kernel(far_ref, ut_ref, top_ref, low_hbm, out_hbm, low_ref, out_ref, low_sem, sems):
    n, step = out_ref.shape[0], 128
    top = top_ref.shape[0]
    low_copies = []
    for k in range((n - top) // step):
        part = slice(k * step, (k + 1) * step)
        low_copies.append(pltpu.make_async_copy(low_hbm.at[part], low_ref.at[part], low_sem.at[k]))
        low_copies[k].start()
    far = far_ref[...].astype(BF16)
    copies = []
    for b in range(n // step):
        rows = slice(b * step, (b + 1) * step)
        if b * step >= top:
            low_copies[b - top // step].wait()
        base = top_ref[rows, :] if b * step < top else low_ref[b * step - top : (b + 1) * step - top, :]
        out_ref[rows, :] = (base + dot(ut_ref[rows, :], far)).astype(BF16)
        copies.append(pltpu.make_async_copy(out_ref.at[rows], out_hbm.at[rows], sems.at[b]))
        copies[-1].start()
    for copy in copies:
        copy.wait()


SMEM = pl.BlockSpec(memory_space=pltpu.SMEM)
VMEM = pl.BlockSpec(memory_space=pltpu.VMEM)
ANY = pl.BlockSpec(memory_space=pl.ANY)
HBM = pl.BlockSpec(memory_space=pltpu.HBM)


def grant(mib):
    return pltpu.CompilerParams(vmem_limit_bytes=mib << 20)


def in_hbm(*arrays):
    return [pltpu.with_memory_space_constraint(a, pltpu.HBM) for a in arrays]


def in_vmem(*arrays):
    return [pltpu.with_memory_space_constraint(a, pltpu.VMEM) for a in arrays]


def shape(dims, dtype=F32):
    return jax.ShapeDtypeStruct(dims, dtype)


def per_device(sources, tree_perm, leaf_blocks, u_factors, v_factors, level_ranks):
    n, rhs = sources.shape
    rank = u_factors.shape[1]
    half = 4 * rank
    low_rows = 512
    core = lax.axis_index("c").reshape(1)
    me = lax.axis_index(MIDDLE).reshape(1)
    perm = tree_perm.reshape(1, n)
    mine, send = pl.pallas_call(
        coef_kernel,
        name="coef",
        in_specs=[SMEM, HBM, HBM, HBM],
        out_specs=[VMEM, VMEM],
        out_shape=[shape((half, rhs)), shape((half + rank, rhs))],
        scratch_shapes=[
            pltpu.VMEM((rhs // 128, 2 * half, 128), F32),
            pltpu.VMEM((1, n), jnp.int32),
            pltpu.VMEM((9, rank, n), BF16),
            pltpu.VMEM((n, rhs), BF16),
            pltpu.SemaphoreType.DMA,
            pltpu.SemaphoreType.DMA,
            pltpu.SemaphoreType.DMA((n // 256,)),
        ],
        compiler_params=grant(14),
    )(core, *in_hbm(perm, v_factors, sources))
    pair = lax.all_gather(send, "c")
    partial = pl.pallas_call(
        add_kernel,
        name="add",
        in_specs=[SMEM, SMEM, VMEM, VMEM],
        out_specs=VMEM,
        out_shape=pltpu.VMEM((half, rhs), F32),
        compiler_params=grant(4),
    )(core, me, *in_vmem(mine, pair)).reshape(8, 16, rhs)
    got = lax.all_to_all(partial, OUTER, 0, 0, tiled=True)
    rows, fine, token = pl.pallas_call(
        middle_kernel,
        name="middle",
        in_specs=[SMEM, VMEM],
        out_specs=[VMEM] * 3,
        out_shape=[shape((32, 2, rhs)), pltpu.VMEM((8, 8, rhs), F32), shape((8, 128))],
        compiler_params=grant(4),
    )(me, got)
    top, low, ut, token = pl.pallas_call(
        local_kernel,
        name="local",
        in_specs=[SMEM, SMEM] + [HBM] * 5 + [VMEM, ANY],
        out_specs=[VMEM, HBM, VMEM, VMEM],
        out_shape=[
            pltpu.VMEM((n - low_rows, rhs), F32),
            pltpu.HBM((low_rows, rhs), F32),
            pltpu.VMEM((n, 2 * half), BF16),
            shape((8, 128)),
        ],
        scratch_shapes=[
            pltpu.VMEM((1, n), jnp.int32),
            pltpu.VMEM((n, rhs), BF16),
            pltpu.VMEM(leaf_blocks.shape, BF16),
            pltpu.VMEM(u_factors.shape, BF16),
            pltpu.VMEM((rank, n), BF16),
            pltpu.VMEM((n, rhs), BF16),
            pltpu.VMEM((n // 128, 2 * half, 128), F32),
            pltpu.VMEM((2 * half, n), BF16),
            pltpu.VMEM((3 * rank, n), BF16),
            pltpu.VMEM((3 * rank, rhs), BF16),
            pltpu.VMEM((low_rows, rhs), F32),
            pltpu.SemaphoreType.DMA((3,)),
            pltpu.SemaphoreType.DMA((n // 256,)),
            pltpu.SemaphoreType.DMA((n // 256,)),
            pltpu.SemaphoreType.DMA((low_rows // 256,)),
        ],
        compiler_params=grant(12),
        cost_estimate=pl.CostEstimate(flops=4_700_000_000, bytes_accessed=8_000_000, transcendentals=0),
    )(level_ranks, core, *in_hbm(perm, sources, leaf_blocks, u_factors, v_factors), *in_vmem(pair), token)
    rows = lax.all_to_all(rows, MIDDLE, 0, 0, tiled=True)
    far = pl.pallas_call(
        far_kernel,
        name="far",
        in_specs=[SMEM, VMEM, VMEM, ANY],
        out_specs=VMEM,
        out_shape=shape((8, 16, rhs)),
        scratch_shapes=[pltpu.VMEM((16, rhs), F32)],
        compiler_params=grant(4),
    )(me, rows, *in_vmem(fine), token)
    far = lax.all_to_all(far, OUTER, 0, 0, tiled=True)
    far = lax.all_gather(far.reshape(half, rhs), "c", axis=0, tiled=True)
    return pl.pallas_call(
        last_kernel,
        name="last",
        in_specs=[VMEM, VMEM, VMEM, HBM],
        out_specs=HBM,
        out_shape=pltpu.HBM((n, rhs), BF16),
        scratch_shapes=[
            pltpu.VMEM((low_rows, rhs), F32),
            pltpu.VMEM((n, rhs), BF16),
            pltpu.SemaphoreType.DMA((low_rows // 128,)),
            pltpu.SemaphoreType.DMA((n // 128,)),
        ],
        compiler_params=grant(8),
    )(*in_vmem(far, ut, top), *in_hbm(low))


def solution(mesh):
    torus = Mesh(mesh.devices.reshape(4, 4, 2, 2, 4, 2), AXES)
    placed = (P(AXES, None), P(AXES), P(AXES, None), P(None, None, AXES), P(None, None, AXES), P())
    return jax.shard_map(
        per_device, mesh=torus, in_specs=placed, out_specs=P(AXES, None), check_vma=False
    )
```

```python
import jax
import jax.numpy as jnp
from jax import lax
from jax.experimental import pallas as pl
from jax.experimental.pallas import tpu as pltpu
from jax.sharding import Mesh
from jax.sharding import PartitionSpec as P

AXES = ("y", "zh", "z1", "z0", "x", "c")
OUTER = ("z0", "x")
MIDDLE = ("y", "zh", "z1")
F32 = jnp.float32
BF16 = jnp.bfloat16
NN = (((1,), (0,)), ((), ()))
NT = (((1,), (1,)), ((), ()))


def dot(a, b, dims=NN):
    return lax.dot_general(a, b, dims, preferred_element_type=F32)


def one_hot_t(perm, first, count):
    n = perm.shape[1]
    j = lax.broadcasted_iota(jnp.int32, (count, n), 0) + first
    return jnp.where(j == perm, 1.0, 0.0).astype(BF16)


def coef_kernel(core, perm_hbm, v_hbm, s_hbm, mine_ref, send_ref, acc, perm_ref, v_ref, s_ref, perm_sem, v_sem, s_sem):
    n = s_ref.shape[0]
    levels, rank, _ = v_ref.shape
    step = 256
    perm_copy = pltpu.make_async_copy(perm_hbm, perm_ref, perm_sem)
    perm_copy.start()
    v_copy = pltpu.make_async_copy(v_hbm.at[0:levels], v_ref, v_sem)
    v_copy.start()

    def s_copy(k):
        rows = pl.ds(pl.multiple_of(k * step, step), step)
        return pltpu.make_async_copy(s_hbm.at[rows], s_ref.at[rows], s_sem.at[k])

    def start(k, _):
        s_copy(k).start()
        return 0

    lax.fori_loop(0, n // step, start, 0)
    perm_copy.wait()
    perm = perm_ref[...] & (n - 1)
    v_copy.wait()
    v = v_ref[...].reshape(levels * rank, n)
    vp = [dot(v, one_hot_t(perm, j, step), NT).astype(BF16) for j in range(0, n, step)]
    for k in range(n // step):
        s_copy(k).wait()
    total = dot(jnp.concatenate(vp, axis=1), s_ref[...])
    half = 4 * rank
    me = core[0]
    mine = pl.ds(pl.multiple_of(me * half, half), half)
    theirs = pl.ds(pl.multiple_of((1 - me) * half, half), half)
    for d in range(acc.shape[0]):
        lanes = slice(d * 128, (d + 1) * 128)
        for level in range(8):
            acc[d, pl.ds(level, rank, stride=8), :] = total[level * rank : (level + 1) * rank, lanes]
        mine_ref[:, lanes] = acc[d, mine, :]
        send_ref[0:half, lanes] = acc[d, theirs, :]
    send_ref[half : half + rank, :] = total[8 * rank : 9 * rank]


def add_kernel(core, _, mine_ref, pair_ref, out_ref):
    half = mine_ref.shape[0]
    out_ref[...] = mine_ref[...] + pair_ref[1 - core[0], 0:half, :]


def local_kernel(
    ranks, core, perm_hbm, s_hbm, leaf_hbm, u_hbm, v_hbm, pair_ref, _,
    top_ref, low_hbm, ut_ref, token_ref,
    perm_ref, s_ref, leaf_ref, u_ref, v_ref, ord_ref, uf_ref, us_ref, ue_ref, fe_ref, low_ref, sems, s_sem, leaf_sem, low_sem,
):
    n, leaf = leaf_ref.shape
    rank = v_ref.shape[0]
    step = 256
    pairs = ((perm_hbm, perm_ref), (u_hbm, u_ref), (v_hbm.at[9], v_ref))
    copies = [pltpu.make_async_copy(a, b, sems.at[k]) for k, (a, b) in enumerate(pairs)]
    for copy in copies:
        copy.start()

    def tall_copies(k):
        rows = pl.ds(pl.multiple_of(k * step, step), step)
        return (
            pltpu.make_async_copy(s_hbm.at[rows], s_ref.at[rows], s_sem.at[k]),
            pltpu.make_async_copy(leaf_hbm.at[rows], leaf_ref.at[rows], leaf_sem.at[k]),
        )

    def start(k, _):
        for copy in tall_copies(k):
            copy.start()
        return 0

    lax.fori_loop(0, n // step, start, 0)
    copies[0].wait()
    perm = perm_ref[...] & (n - 1)
    copies[1].wait()
    row = lax.broadcasted_iota(jnp.int32, (rank, n), 0)
    lane_n = lax.broadcasted_iota(jnp.int32, (rank, n), 1)
    for level in range(8):
        kept = jnp.where(row < ranks[level], u_ref[level].astype(F32), 0.0)
        for d in range(n // 128):
            uf_ref[d, pl.ds(level, rank, stride=8), :] = kept[:, d * 128 : (d + 1) * 128]
    for d in range(n // 128):
        us_ref[:, d * 128 : (d + 1) * 128] = uf_ref[d].astype(BF16)
    ue_ref[0:rank, :] = jnp.where(row < ranks[8], u_ref[8].astype(F32), 0.0).astype(BF16)
    last = jnp.where(row < ranks[9], u_ref[9].astype(F32), 0.0)
    ue_ref[rank : 2 * rank, :] = jnp.where(lane_n < leaf, last, 0.0).astype(BF16)
    ue_ref[2 * rank : 3 * rank, :] = jnp.where(lane_n < leaf, 0.0, last).astype(BF16)

    copies[2].wait()
    for k in range(n // step):
        for copy in tall_copies(k):
            copy.wait()
    lane = lax.broadcasted_iota(jnp.int32, (128, 128), 1)
    for i in range(0, n, step):
        hot = []
        for h in range(i, i + step, 128):
            column = jnp.broadcast_to(perm[:, h : h + 128], (128, 128)).T
            hot.append(
                jnp.concatenate(
                    [jnp.where(column == lane + j, 1.0, 0.0).astype(BF16) for j in range(0, n, 128)], axis=1
                )
            )
        ord_ref[i : i + step, :] = dot(jnp.concatenate(hot, axis=0), s_ref[...]).astype(BF16)
    fe_ref[0:rank, :] = pair_ref[1 - core[0], 4 * rank :, :].astype(BF16)
    fe_ref[rank : 2 * rank, :] = dot(v_ref[:, leaf:], ord_ref[leaf:, :]).astype(BF16)
    fe_ref[2 * rank : 3 * rank, :] = dot(v_ref[:, :leaf], ord_ref[:leaf, :]).astype(BF16)
    top = top_ref.shape[0]
    kept = []
    for j in [*range(top, n, step), *range(0, top, step)]:
        rows = slice(j, j + step)
        hot = one_hot_t(perm, j, step)
        leaves = [dot(hot[:, g : g + leaf], leaf_ref[g : g + leaf, :]).astype(BF16) for g in range(0, n, leaf)]
        ut_ref[rows, :] = dot(hot, us_ref[...], NT).astype(BF16)
        et = dot(hot, ue_ref[...], NT).astype(BF16)
        base = dot(jnp.concatenate(leaves, axis=1), ord_ref[...]) + dot(et, fe_ref[...])
        if j < top:
            top_ref[rows, :] = base
        else:
            part = slice(j - top, j - top + step)
            low_ref[part, :] = base
            kept.append(pltpu.make_async_copy(low_ref.at[part], low_hbm.at[part], low_sem.at[len(kept)]))
            kept[-1].start()
    token_ref[...] = jnp.zeros_like(token_ref)
    for copy in kept:
        copy.wait()


def level_at(apart):
    for bit, row in ((16, 0), (8, 1), (4, 2), (2, 3)):
        if apart & bit:
            return row
    return 4


def middle_kernel(me, got_ref, out_ref, fine_ref, token_ref):
    token_ref[...] = jnp.zeros_like(token_ref)
    rows = got_ref.shape[1]
    got = lambda z, x: got_ref[z * 4 + x]
    sums = [(got(z, 0) + got(z, 1)) + (got(z, 2) + got(z, 3)) for z in range(2)]
    total = sums[0] + sums[1]
    for z in range(2):
        for x in range(4):
            for j in range(rows // 8):
                at = lambda a, row: a[j * 8 + row : j * 8 + row + 1]
                fine_ref[z * 4 + x, j * 4 : j * 4 + 1, :] = at(sums[z ^ 1], 5)
                fine_ref[z * 4 + x, j * 4 + 1 : j * 4 + 2, :] = at(got(z, x ^ 2), 6) + at(got(z, x ^ 3), 6)
                fine_ref[z * 4 + x, j * 4 + 2 : j * 4 + 3, :] = at(got(z, x ^ 1), 7)
    for row in range(5):
        sent = jnp.concatenate([total[r + row : r + row + 1] for r in range(0, rows, 8)], axis=0)
        for apart in range(out_ref.shape[0]):
            if level_at(apart) == row:
                out_ref[me[0] ^ apart] = sent


def far_kernel(me, got_ref, fine_ref, _, out_ref, acc):
    rows = acc.shape[0]
    acc[...] = jnp.zeros_like(acc)
    for row in range(5):
        parts = [got_ref[me[0] ^ k] for k in range(1, got_ref.shape[0]) if level_at(k) == row]
        while len(parts) > 1:
            parts = [sum(parts[k : k + 2]) for k in range(0, len(parts), 2)]
        for j in range(rows // 8):
            acc[j * 8 + row : j * 8 + row + 1, :] = parts[0][j : j + 1]
    far = acc[...]
    for p in range(out_ref.shape[0]):
        out_ref[p] = far
        for j in range(rows // 8):
            out_ref[p, j * 8 + 5 : j * 8 + 8, :] = fine_ref[p, j * 4 : j * 4 + 3, :]


def last_kernel(far_ref, ut_ref, top_ref, low_ref, out_hbm, out_ref, sems):
    n, step = out_ref.shape[0], 128
    top = top_ref.shape[0]
    far = far_ref[...].astype(BF16)
    copies = []
    for b in range(n // step):
        rows = slice(b * step, (b + 1) * step)
        base = top_ref[rows, :] if b * step < top else low_ref[b * step - top : (b + 1) * step - top, :]
        out_ref[rows, :] = (base + dot(ut_ref[rows, :], far)).astype(BF16)
        copies.append(pltpu.make_async_copy(out_ref.at[rows], out_hbm.at[rows], sems.at[b]))
        copies[-1].start()
    for copy in copies:
        copy.wait()


SMEM = pl.BlockSpec(memory_space=pltpu.SMEM)
VMEM = pl.BlockSpec(memory_space=pltpu.VMEM)
ANY = pl.BlockSpec(memory_space=pl.ANY)
HBM = pl.BlockSpec(memory_space=pltpu.HBM)


def grant(mib):
    return pltpu.CompilerParams(vmem_limit_bytes=mib << 20)


def in_hbm(*arrays):
    return [pltpu.with_memory_space_constraint(a, pltpu.HBM) for a in arrays]


def in_vmem(*arrays):
    return [pltpu.with_memory_space_constraint(a, pltpu.VMEM) for a in arrays]


def shape(dims, dtype=F32):
    return jax.ShapeDtypeStruct(dims, dtype)


def per_device(sources, tree_perm, leaf_blocks, u_factors, v_factors, level_ranks):
    n, rhs = sources.shape
    rank = u_factors.shape[1]
    half = 4 * rank
    low_rows = 768
    core = lax.axis_index("c").reshape(1)
    me = lax.axis_index(MIDDLE).reshape(1)
    perm = tree_perm.reshape(1, n)
    mine, send = pl.pallas_call(
        coef_kernel,
        name="coef",
        in_specs=[SMEM, HBM, HBM, HBM],
        out_specs=[VMEM, VMEM],
        out_shape=[shape((half, rhs)), shape((half + rank, rhs))],
        scratch_shapes=[
            pltpu.VMEM((rhs // 128, 2 * half, 128), F32),
            pltpu.VMEM((1, n), jnp.int32),
            pltpu.VMEM((9, rank, n), BF16),
            pltpu.VMEM((n, rhs), BF16),
            pltpu.SemaphoreType.DMA,
            pltpu.SemaphoreType.DMA,
            pltpu.SemaphoreType.DMA((n // 256,)),
        ],
        compiler_params=grant(14),
    )(core, *in_hbm(perm, v_factors, sources))
    pair = lax.all_gather(send, "c")
    partial = pl.pallas_call(
        add_kernel,
        name="add",
        in_specs=[SMEM, SMEM, VMEM, VMEM],
        out_specs=VMEM,
        out_shape=pltpu.VMEM((half, rhs), F32),
        compiler_params=grant(4),
    )(core, me, *in_vmem(mine, pair)).reshape(8, 16, rhs)
    got = lax.all_to_all(partial, OUTER, 0, 0, tiled=True)
    rows, fine, token = pl.pallas_call(
        middle_kernel,
        name="middle",
        in_specs=[SMEM, VMEM],
        out_specs=[VMEM] * 3,
        out_shape=[shape((32, 2, rhs)), pltpu.VMEM((8, 8, rhs), F32), shape((8, 128))],
        compiler_params=grant(4),
    )(me, got)
    top, low, ut, token = pl.pallas_call(
        local_kernel,
        name="local",
        in_specs=[SMEM, SMEM] + [HBM] * 5 + [VMEM, ANY],
        out_specs=[VMEM, HBM, VMEM, VMEM],
        out_shape=[
            pltpu.VMEM((n - low_rows, rhs), F32),
            pltpu.HBM((low_rows, rhs), F32),
            pltpu.VMEM((n, 2 * half), BF16),
            shape((8, 128)),
        ],
        scratch_shapes=[
            pltpu.VMEM((1, n), jnp.int32),
            pltpu.VMEM((n, rhs), BF16),
            pltpu.VMEM(leaf_blocks.shape, BF16),
            pltpu.VMEM(u_factors.shape, BF16),
            pltpu.VMEM((rank, n), BF16),
            pltpu.VMEM((n, rhs), BF16),
            pltpu.VMEM((n // 128, 2 * half, 128), F32),
            pltpu.VMEM((2 * half, n), BF16),
            pltpu.VMEM((3 * rank, n), BF16),
            pltpu.VMEM((3 * rank, rhs), BF16),
            pltpu.VMEM((low_rows, rhs), F32),
            pltpu.SemaphoreType.DMA((3,)),
            pltpu.SemaphoreType.DMA((n // 256,)),
            pltpu.SemaphoreType.DMA((n // 256,)),
            pltpu.SemaphoreType.DMA((low_rows // 256,)),
        ],
        compiler_params=grant(12),
        cost_estimate=pl.CostEstimate(flops=4_700_000_000, bytes_accessed=8_000_000, transcendentals=0),
    )(level_ranks, core, *in_hbm(perm, sources, leaf_blocks, u_factors, v_factors), *in_vmem(pair), token)
    rows = lax.all_to_all(rows, MIDDLE, 0, 0, tiled=True)
    far = pl.pallas_call(
        far_kernel,
        name="far",
        in_specs=[SMEM, VMEM, VMEM, ANY],
        out_specs=VMEM,
        out_shape=shape((8, 16, rhs)),
        scratch_shapes=[pltpu.VMEM((16, rhs), F32)],
        compiler_params=grant(4),
    )(me, rows, *in_vmem(fine), token)
    far = lax.all_to_all(far, OUTER, 0, 0, tiled=True)
    far = lax.all_gather(far.reshape(half, rhs), "c", axis=0, tiled=True)
    return pl.pallas_call(
        last_kernel,
        name="last",
        in_specs=[VMEM] * 4,
        out_specs=HBM,
        out_shape=pltpu.HBM((n, rhs), BF16),
        scratch_shapes=[
            pltpu.VMEM((n, rhs), BF16),
            pltpu.SemaphoreType.DMA((n // 128,)),
        ],
        compiler_params=grant(8),
    )(*in_vmem(far, ut, top, low))


def solution(mesh):
    torus = Mesh(mesh.devices.reshape(4, 4, 2, 2, 4, 2), AXES)
    placed = (P(AXES, None), P(AXES), P(AXES, None), P(None, None, AXES), P(None, None, AXES), P())
    return jax.shard_map(
        per_device, mesh=torus, in_specs=placed, out_specs=P(AXES, None), check_vma=False
    )
```

```python
import jax
import jax.numpy as jnp
from jax import lax
from jax.experimental import pallas as pl
from jax.experimental.pallas import tpu as pltpu
from jax.sharding import Mesh
from jax.sharding import PartitionSpec as P

AXES = ("y", "zh", "z1", "z0", "x", "c")
OUTER = ("z0", "x")
MIDDLE = ("zh", "y", "z1")
F32 = jnp.float32
BF16 = jnp.bfloat16
NN = (((1,), (0,)), ((), ()))
NT = (((1,), (1,)), ((), ()))


def dot(a, b, dims=NN):
    return lax.dot_general(a, b, dims, preferred_element_type=F32)


def one_hot_t(perm, first, count):
    n = perm.shape[1]
    j = lax.broadcasted_iota(jnp.int32, (count, n), 0) + first
    return jnp.where(j == perm, 1.0, 0.0).astype(BF16)


def coef_kernel(core, perm_hbm, v_hbm, s_hbm, mine_ref, send_ref, acc, perm_ref, v_ref, s_ref, perm_sem, v_sem, s_sem):
    n = s_ref.shape[0]
    levels, rank, _ = v_ref.shape
    step = 256
    perm_copy = pltpu.make_async_copy(perm_hbm, perm_ref, perm_sem)
    perm_copy.start()
    v_copy = pltpu.make_async_copy(v_hbm.at[0:levels], v_ref, v_sem)
    v_copy.start()

    def s_copy(k):
        rows = pl.ds(pl.multiple_of(k * step, step), step)
        return pltpu.make_async_copy(s_hbm.at[rows], s_ref.at[rows], s_sem.at[k])

    def start(k, _):
        s_copy(k).start()
        return 0

    lax.fori_loop(0, n // step, start, 0)
    perm_copy.wait()
    perm = perm_ref[...] & (n - 1)
    v_copy.wait()
    v = v_ref[...].reshape(levels * rank, n)
    vp = [dot(v, one_hot_t(perm, j, step), NT).astype(BF16) for j in range(0, n, step)]
    for k in range(n // step):
        s_copy(k).wait()
    total = dot(jnp.concatenate(vp, axis=1), s_ref[...])
    half = 4 * rank
    me = core[0]
    mine = pl.ds(pl.multiple_of(me * half, half), half)
    theirs = pl.ds(pl.multiple_of((1 - me) * half, half), half)
    for d in range(acc.shape[0]):
        lanes = slice(d * 128, (d + 1) * 128)
        for level in range(8):
            acc[d, pl.ds(level, rank, stride=8), :] = total[level * rank : (level + 1) * rank, lanes]
        mine_ref[:, lanes] = acc[d, mine, :]
        send_ref[0:half, lanes] = acc[d, theirs, :]
    send_ref[half : half + rank, :] = total[8 * rank : 9 * rank]


def add_kernel(core, _, mine_ref, pair_ref, out_ref):
    half = mine_ref.shape[0]
    out_ref[...] = mine_ref[...] + pair_ref[1 - core[0], 0:half, :]


def local_kernel(
    ranks, core, perm_hbm, s_hbm, leaf_hbm, u_hbm, v_hbm, pair_ref, _,
    top_ref, low_hbm, ut_ref, token_ref,
    perm_ref, s_ref, leaf_ref, u_ref, v_ref, ord_ref, uf_ref, us_ref, ue_ref, fe_ref, low_ref, sems, s_sem, leaf_sem, low_sem,
):
    n, leaf = leaf_ref.shape
    rank = v_ref.shape[0]
    step = 256
    pairs = ((perm_hbm, perm_ref), (u_hbm, u_ref), (v_hbm.at[9], v_ref))
    copies = [pltpu.make_async_copy(a, b, sems.at[k]) for k, (a, b) in enumerate(pairs)]
    for copy in copies:
        copy.start()

    def tall_copies(k):
        rows = pl.ds(pl.multiple_of(k * step, step), step)
        return (
            pltpu.make_async_copy(s_hbm.at[rows], s_ref.at[rows], s_sem.at[k]),
            pltpu.make_async_copy(leaf_hbm.at[rows], leaf_ref.at[rows], leaf_sem.at[k]),
        )

    def start(k, _):
        for copy in tall_copies(k):
            copy.start()
        return 0

    lax.fori_loop(0, n // step, start, 0)
    copies[0].wait()
    perm = perm_ref[...] & (n - 1)
    copies[1].wait()
    row = lax.broadcasted_iota(jnp.int32, (rank, n), 0)
    lane_n = lax.broadcasted_iota(jnp.int32, (rank, n), 1)
    for level in range(8):
        kept = jnp.where(row < ranks[level], u_ref[level].astype(F32), 0.0)
        for d in range(n // 128):
            uf_ref[d, pl.ds(level, rank, stride=8), :] = kept[:, d * 128 : (d + 1) * 128]
    for d in range(n // 128):
        us_ref[:, d * 128 : (d + 1) * 128] = uf_ref[d].astype(BF16)
    ue_ref[0:rank, :] = jnp.where(row < ranks[8], u_ref[8].astype(F32), 0.0).astype(BF16)
    last = jnp.where(row < ranks[9], u_ref[9].astype(F32), 0.0)
    ue_ref[rank : 2 * rank, :] = jnp.where(lane_n < leaf, last, 0.0).astype(BF16)
    ue_ref[2 * rank : 3 * rank, :] = jnp.where(lane_n < leaf, 0.0, last).astype(BF16)

    copies[2].wait()
    for k in range(n // step):
        for copy in tall_copies(k):
            copy.wait()
    lane = lax.broadcasted_iota(jnp.int32, (128, 128), 1)
    for i in range(0, n, step):
        hot = []
        for h in range(i, i + step, 128):
            column = jnp.broadcast_to(perm[:, h : h + 128], (128, 128)).T
            hot.append(
                jnp.concatenate(
                    [jnp.where(column == lane + j, 1.0, 0.0).astype(BF16) for j in range(0, n, 128)], axis=1
                )
            )
        ord_ref[i : i + step, :] = dot(jnp.concatenate(hot, axis=0), s_ref[...]).astype(BF16)
    fe_ref[0:rank, :] = pair_ref[1 - core[0], 4 * rank :, :].astype(BF16)
    fe_ref[rank : 2 * rank, :] = dot(v_ref[:, leaf:], ord_ref[leaf:, :]).astype(BF16)
    fe_ref[2 * rank : 3 * rank, :] = dot(v_ref[:, :leaf], ord_ref[:leaf, :]).astype(BF16)
    top = top_ref.shape[0]
    kept = []
    for j in [*range(top, n, step), *range(0, top, step)]:
        rows = slice(j, j + step)
        hot = one_hot_t(perm, j, step)
        leaves = [dot(hot[:, g : g + leaf], leaf_ref[g : g + leaf, :]).astype(BF16) for g in range(0, n, leaf)]
        ut_ref[rows, :] = dot(hot, us_ref[...], NT).astype(BF16)
        et = dot(hot, ue_ref[...], NT).astype(BF16)
        base = dot(jnp.concatenate(leaves, axis=1), ord_ref[...]) + dot(et, fe_ref[...])
        if j < top:
            top_ref[rows, :] = base
        else:
            part = slice(j - top, j - top + step)
            low_ref[part, :] = base
            kept.append(pltpu.make_async_copy(low_ref.at[part], low_hbm.at[part], low_sem.at[len(kept)]))
            kept[-1].start()
    token_ref[...] = jnp.zeros_like(token_ref)
    for copy in kept:
        copy.wait()


def level_at(apart):
    for bit, row in ((4, 0), (2, 1), (16, 2), (8, 3)):
        if apart & bit:
            return row
    return 4


def middle_kernel(me, got_ref, out_ref, fine_ref, token_ref):
    token_ref[...] = jnp.zeros_like(token_ref)
    rows = got_ref.shape[1]
    got = lambda z, x: got_ref[z * 4 + x]
    sums = [(got(z, 0) + got(z, 1)) + (got(z, 2) + got(z, 3)) for z in range(2)]
    total = sums[0] + sums[1]
    for z in range(2):
        for x in range(4):
            for j in range(rows // 8):
                at = lambda a, row: a[j * 8 + row : j * 8 + row + 1]
                fine_ref[z * 4 + x, j * 4 : j * 4 + 1, :] = at(sums[z ^ 1], 5)
                fine_ref[z * 4 + x, j * 4 + 1 : j * 4 + 2, :] = at(got(z, x ^ 2), 6) + at(got(z, x ^ 3), 6)
                fine_ref[z * 4 + x, j * 4 + 2 : j * 4 + 3, :] = at(got(z, x ^ 1), 7)
    for row in range(5):
        sent = jnp.concatenate([total[r + row : r + row + 1] for r in range(0, rows, 8)], axis=0)
        for apart in range(out_ref.shape[0]):
            if level_at(apart) == row:
                out_ref[me[0] ^ apart] = sent


def far_kernel(me, got_ref, fine_ref, _, out_ref, acc):
    rows = acc.shape[0]
    acc[...] = jnp.zeros_like(acc)
    for row in range(5):
        parts = [got_ref[me[0] ^ k] for k in range(1, got_ref.shape[0]) if level_at(k) == row]
        while len(parts) > 1:
            parts = [sum(parts[k : k + 2]) for k in range(0, len(parts), 2)]
        for j in range(rows // 8):
            acc[j * 8 + row : j * 8 + row + 1, :] = parts[0][j : j + 1]
    far = acc[...]
    for p in range(out_ref.shape[0]):
        out_ref[p] = far
        for j in range(rows // 8):
            out_ref[p, j * 8 + 5 : j * 8 + 8, :] = fine_ref[p, j * 4 : j * 4 + 3, :]


def last_kernel(far_ref, ut_ref, top_ref, low_ref, out_hbm, out_ref, sems):
    n, step = out_ref.shape[0], 128
    top = top_ref.shape[0]
    far = far_ref[...].astype(BF16)
    copies = []
    for b in range(n // step):
        rows = slice(b * step, (b + 1) * step)
        base = top_ref[rows, :] if b * step < top else low_ref[b * step - top : (b + 1) * step - top, :]
        out_ref[rows, :] = (base + dot(ut_ref[rows, :], far)).astype(BF16)
        copies.append(pltpu.make_async_copy(out_ref.at[rows], out_hbm.at[rows], sems.at[b]))
        copies[-1].start()
    for copy in copies:
        copy.wait()


SMEM = pl.BlockSpec(memory_space=pltpu.SMEM)
VMEM = pl.BlockSpec(memory_space=pltpu.VMEM)
ANY = pl.BlockSpec(memory_space=pl.ANY)
HBM = pl.BlockSpec(memory_space=pltpu.HBM)


def grant(mib):
    return pltpu.CompilerParams(vmem_limit_bytes=mib << 20)


def in_hbm(*arrays):
    return [pltpu.with_memory_space_constraint(a, pltpu.HBM) for a in arrays]


def in_vmem(*arrays):
    return [pltpu.with_memory_space_constraint(a, pltpu.VMEM) for a in arrays]


def shape(dims, dtype=F32):
    return jax.ShapeDtypeStruct(dims, dtype)


def per_device(sources, tree_perm, leaf_blocks, u_factors, v_factors, level_ranks):
    n, rhs = sources.shape
    rank = u_factors.shape[1]
    half = 4 * rank
    low_rows = 768
    core = lax.axis_index("c").reshape(1)
    me = lax.axis_index(MIDDLE).reshape(1)
    perm = tree_perm.reshape(1, n)
    mine, send = pl.pallas_call(
        coef_kernel,
        name="coef",
        in_specs=[SMEM, HBM, HBM, HBM],
        out_specs=[VMEM, VMEM],
        out_shape=[shape((half, rhs)), shape((half + rank, rhs))],
        scratch_shapes=[
            pltpu.VMEM((rhs // 128, 2 * half, 128), F32),
            pltpu.VMEM((1, n), jnp.int32),
            pltpu.VMEM((9, rank, n), BF16),
            pltpu.VMEM((n, rhs), BF16),
            pltpu.SemaphoreType.DMA,
            pltpu.SemaphoreType.DMA,
            pltpu.SemaphoreType.DMA((n // 256,)),
        ],
        compiler_params=grant(14),
    )(core, *in_hbm(perm, v_factors, sources))
    pair = lax.all_gather(send, "c")
    partial = pl.pallas_call(
        add_kernel,
        name="add",
        in_specs=[SMEM, SMEM, VMEM, VMEM],
        out_specs=VMEM,
        out_shape=pltpu.VMEM((half, rhs), F32),
        compiler_params=grant(4),
    )(core, me, *in_vmem(mine, pair)).reshape(8, 16, rhs)
    got = lax.all_to_all(partial, OUTER, 0, 0, tiled=True)
    rows, fine, token = pl.pallas_call(
        middle_kernel,
        name="middle",
        in_specs=[SMEM, VMEM],
        out_specs=[VMEM] * 3,
        out_shape=[shape((32, 2, rhs)), pltpu.VMEM((8, 8, rhs), F32), shape((8, 128))],
        compiler_params=grant(4),
    )(me, got)
    top, low, ut, token = pl.pallas_call(
        local_kernel,
        name="local",
        in_specs=[SMEM, SMEM] + [HBM] * 5 + [VMEM, ANY],
        out_specs=[VMEM, HBM, VMEM, VMEM],
        out_shape=[
            pltpu.VMEM((n - low_rows, rhs), F32),
            pltpu.HBM((low_rows, rhs), F32),
            pltpu.VMEM((n, 2 * half), BF16),
            shape((8, 128)),
        ],
        scratch_shapes=[
            pltpu.VMEM((1, n), jnp.int32),
            pltpu.VMEM((n, rhs), BF16),
            pltpu.VMEM(leaf_blocks.shape, BF16),
            pltpu.VMEM(u_factors.shape, BF16),
            pltpu.VMEM((rank, n), BF16),
            pltpu.VMEM((n, rhs), BF16),
            pltpu.VMEM((n // 128, 2 * half, 128), F32),
            pltpu.VMEM((2 * half, n), BF16),
            pltpu.VMEM((3 * rank, n), BF16),
            pltpu.VMEM((3 * rank, rhs), BF16),
            pltpu.VMEM((low_rows, rhs), F32),
            pltpu.SemaphoreType.DMA((3,)),
            pltpu.SemaphoreType.DMA((n // 256,)),
            pltpu.SemaphoreType.DMA((n // 256,)),
            pltpu.SemaphoreType.DMA((low_rows // 256,)),
        ],
        compiler_params=grant(12),
        cost_estimate=pl.CostEstimate(flops=4_700_000_000, bytes_accessed=8_000_000, transcendentals=0),
    )(level_ranks, core, *in_hbm(perm, sources, leaf_blocks, u_factors, v_factors), *in_vmem(pair), token)
    rows = lax.all_to_all(rows, MIDDLE, 0, 0, tiled=True)
    far = pl.pallas_call(
        far_kernel,
        name="far",
        in_specs=[SMEM, VMEM, VMEM, ANY],
        out_specs=VMEM,
        out_shape=shape((8, 16, rhs)),
        scratch_shapes=[pltpu.VMEM((16, rhs), F32)],
        compiler_params=grant(4),
    )(me, rows, *in_vmem(fine), token)
    far = lax.all_to_all(far, OUTER, 0, 0, tiled=True)
    far = lax.all_gather(far.reshape(half, rhs), "c", axis=0, tiled=True)
    return pl.pallas_call(
        last_kernel,
        name="last",
        in_specs=[VMEM] * 4,
        out_specs=HBM,
        out_shape=pltpu.HBM((n, rhs), BF16),
        scratch_shapes=[
            pltpu.VMEM((n, rhs), BF16),
            pltpu.SemaphoreType.DMA((n // 128,)),
        ],
        compiler_params=grant(8),
    )(*in_vmem(far, ut, top, low))


def solution(mesh):
    torus = Mesh(mesh.devices.reshape(4, 4, 2, 2, 4, 2), AXES)
    placed = (P(AXES, None), P(AXES), P(AXES, None), P(None, None, AXES), P(None, None, AXES), P())
    return jax.shard_map(
        per_device, mesh=torus, in_specs=placed, out_specs=P(AXES, None), check_vma=False
    )
```

```python
import jax
import jax.numpy as jnp
from jax import lax
from jax.experimental import pallas as pl
from jax.experimental.pallas import tpu as pltpu
from jax.sharding import Mesh
from jax.sharding import PartitionSpec as P

AXES = ("y", "zh", "z1", "z0", "x", "c")
OUTER = ("z0", "x")
MIDDLE = ("y", "zh", "z1")
F32 = jnp.float32
BF16 = jnp.bfloat16
NN = (((1,), (0,)), ((), ()))
NT = (((1,), (1,)), ((), ()))


def dot(a, b, dims=NN):
    return lax.dot_general(a, b, dims, preferred_element_type=F32)


def one_hot_t(perm, first, count):
    n = perm.shape[1]
    j = lax.broadcasted_iota(jnp.int32, (count, n), 0) + first
    return jnp.where(j == perm, 1.0, 0.0).astype(BF16)


def coef_kernel(core, perm_hbm, v_hbm, s_hbm, mine_ref, send_ref, acc, perm_ref, v_ref, s_ref, perm_sem, v_sem, s_sem):
    n = s_ref.shape[0]
    levels, rank, _ = v_ref.shape
    step = 256
    perm_copy = pltpu.make_async_copy(perm_hbm, perm_ref, perm_sem)
    perm_copy.start()
    v_copy = pltpu.make_async_copy(v_hbm.at[0:levels], v_ref, v_sem)
    v_copy.start()

    def s_copy(k):
        rows = pl.ds(pl.multiple_of(k * step, step), step)
        return pltpu.make_async_copy(s_hbm.at[rows], s_ref.at[rows], s_sem.at[k])

    def start(k, _):
        s_copy(k).start()
        return 0

    lax.fori_loop(0, n // step, start, 0)
    perm_copy.wait()
    perm = perm_ref[...] & (n - 1)
    v_copy.wait()
    v = v_ref[...].reshape(levels * rank, n)
    vp = [dot(v, one_hot_t(perm, j, step), NT).astype(BF16) for j in range(0, n, step)]
    for k in range(n // step):
        s_copy(k).wait()
    total = dot(jnp.concatenate(vp, axis=1), s_ref[...])
    half = 4 * rank
    me = core[0]
    mine = pl.ds(pl.multiple_of(me * half, half), half)
    theirs = pl.ds(pl.multiple_of((1 - me) * half, half), half)
    for d in range(acc.shape[0]):
        lanes = slice(d * 128, (d + 1) * 128)
        for level in range(8):
            acc[d, pl.ds(level, rank, stride=8), :] = total[level * rank : (level + 1) * rank, lanes]
        mine_ref[:, lanes] = acc[d, mine, :]
        send_ref[0:half, lanes] = acc[d, theirs, :]
    send_ref[half : half + rank, :] = total[8 * rank : 9 * rank]


def add_kernel(core, _, mine_ref, pair_ref, out_ref):
    half = mine_ref.shape[0]
    out_ref[...] = mine_ref[...] + pair_ref[1 - core[0], 0:half, :]


def local_kernel(
    ranks, core, perm_ref, s_hbm, leaf_hbm, u_hbm, v_hbm, pair_ref, _,
    top_ref, low_hbm, ut_ref, token_ref,
    s_ref, leaf_ref, u_ref, v_ref, ord_ref, uf_ref, us_ref, ue_ref, fe_ref, low_ref, sems, s_sem, leaf_sem, low_sem,
):
    n, leaf = leaf_ref.shape
    rank = v_ref.shape[0]
    step = 256
    u_copy = pltpu.make_async_copy(u_hbm, u_ref, sems.at[0])
    v_copy = pltpu.make_async_copy(v_hbm.at[9], v_ref, sems.at[1])

    def s_copy(k):
        rows = pl.ds(pl.multiple_of(k * step, step), step)
        return pltpu.make_async_copy(s_hbm.at[rows], s_ref.at[rows], s_sem.at[k])

    def leaf_copy(k):
        rows = pl.ds(pl.multiple_of(k * step, step), step)
        return pltpu.make_async_copy(leaf_hbm.at[rows], leaf_ref.at[rows], leaf_sem.at[k])

    def start_s(k, _):
        s_copy(k).start()
        return 0

    def start_leaf(k, _):
        leaf_copy(k).start()
        return 0

    lax.fori_loop(0, n // step, start_s, 0)
    v_copy.start()
    u_copy.start()
    lax.fori_loop(0, n // step, start_leaf, 0)
    perm = perm_ref[...] & (n - 1)
    lane = lax.broadcasted_iota(jnp.int32, (128, 128), 1)

    def one_hot(i):
        hot = []
        for h in range(i, i + step, 128):
            column = jnp.broadcast_to(perm[:, h : h + 128], (128, 128)).T
            hot.append(
                jnp.concatenate(
                    [jnp.where(column == lane + j, 1.0, 0.0).astype(BF16) for j in range(0, n, 128)], axis=1
                )
            )
        return jnp.concatenate(hot, axis=0)

    hot = one_hot(0)
    for k in range(n // step):
        s_copy(k).wait()
    for i in range(0, n, step):
        ord_ref[i : i + step, :] = dot(hot, s_ref[...]).astype(BF16)
        if i + step < n:
            hot = one_hot(i + step)
    u_copy.wait()
    row = lax.broadcasted_iota(jnp.int32, (rank, n), 0)
    lane_n = lax.broadcasted_iota(jnp.int32, (rank, n), 1)
    for level in range(8):
        kept = jnp.where(row < ranks[level], u_ref[level].astype(F32), 0.0)
        for d in range(n // 128):
            uf_ref[d, pl.ds(level, rank, stride=8), :] = kept[:, d * 128 : (d + 1) * 128]
    for d in range(n // 128):
        us_ref[:, d * 128 : (d + 1) * 128] = uf_ref[d].astype(BF16)
    ue_ref[0:rank, :] = jnp.where(row < ranks[8], u_ref[8].astype(F32), 0.0).astype(BF16)
    last = jnp.where(row < ranks[9], u_ref[9].astype(F32), 0.0)
    ue_ref[rank : 2 * rank, :] = jnp.where(lane_n < leaf, last, 0.0).astype(BF16)
    ue_ref[2 * rank : 3 * rank, :] = jnp.where(lane_n < leaf, 0.0, last).astype(BF16)

    v_copy.wait()
    for k in range(n // step):
        leaf_copy(k).wait()
    fe_ref[0:rank, :] = pair_ref[1 - core[0], 4 * rank :, :].astype(BF16)
    fe_ref[rank : 2 * rank, :] = dot(v_ref[:, leaf:], ord_ref[leaf:, :]).astype(BF16)
    fe_ref[2 * rank : 3 * rank, :] = dot(v_ref[:, :leaf], ord_ref[:leaf, :]).astype(BF16)
    top = top_ref.shape[0]
    kept = []
    for j in [*range(top, n, step), *range(0, top, step)]:
        rows = slice(j, j + step)
        hot = one_hot_t(perm, j, step)
        leaves = [dot(hot[:, g : g + leaf], leaf_ref[g : g + leaf, :]).astype(BF16) for g in range(0, n, leaf)]
        ut_ref[rows, :] = dot(hot, us_ref[...], NT).astype(BF16)
        et = dot(hot, ue_ref[...], NT).astype(BF16)
        base = dot(jnp.concatenate(leaves, axis=1), ord_ref[...]) + dot(et, fe_ref[...])
        if j < top:
            top_ref[rows, :] = base
        else:
            part = slice(j - top, j - top + step)
            low_ref[part, :] = base
            kept.append(pltpu.make_async_copy(low_ref.at[part], low_hbm.at[part], low_sem.at[len(kept)]))
            kept[-1].start()
    token_ref[...] = jnp.zeros_like(token_ref)
    for copy in kept:
        copy.wait()


def level_at(apart):
    for bit, row in ((16, 0), (8, 1), (4, 2), (2, 3)):
        if apart & bit:
            return row
    return 4


def middle_kernel(me, got_ref, out_ref, fine_ref, token_ref):
    token_ref[...] = jnp.zeros_like(token_ref)
    rows = got_ref.shape[1]
    got = lambda z, x: got_ref[z * 4 + x]
    sums = [(got(z, 0) + got(z, 1)) + (got(z, 2) + got(z, 3)) for z in range(2)]
    total = sums[0] + sums[1]
    for z in range(2):
        for x in range(4):
            for j in range(rows // 8):
                at = lambda a, row: a[j * 8 + row : j * 8 + row + 1]
                fine_ref[z * 4 + x, j * 4 : j * 4 + 1, :] = at(sums[z ^ 1], 5)
                fine_ref[z * 4 + x, j * 4 + 1 : j * 4 + 2, :] = at(got(z, x ^ 2), 6) + at(got(z, x ^ 3), 6)
                fine_ref[z * 4 + x, j * 4 + 2 : j * 4 + 3, :] = at(got(z, x ^ 1), 7)
    for row in range(5):
        sent = jnp.concatenate([total[r + row : r + row + 1] for r in range(0, rows, 8)], axis=0)
        for apart in range(out_ref.shape[0]):
            if level_at(apart) == row:
                out_ref[me[0] ^ apart] = sent


def far_kernel(me, got_ref, fine_ref, _, out_ref, acc):
    rows = acc.shape[0]
    acc[...] = jnp.zeros_like(acc)
    for row in range(5):
        parts = [got_ref[me[0] ^ k] for k in range(1, got_ref.shape[0]) if level_at(k) == row]
        while len(parts) > 1:
            parts = [sum(parts[k : k + 2]) for k in range(0, len(parts), 2)]
        for j in range(rows // 8):
            acc[j * 8 + row : j * 8 + row + 1, :] = parts[0][j : j + 1]
    far = acc[...]
    for p in range(out_ref.shape[0]):
        out_ref[p] = far
        for j in range(rows // 8):
            out_ref[p, j * 8 + 5 : j * 8 + 8, :] = fine_ref[p, j * 4 : j * 4 + 3, :]


def last_kernel(far_ref, ut_ref, top_ref, low_ref, out_hbm, out_ref, sems):
    n, step = out_ref.shape[0], 128
    top = top_ref.shape[0]
    far = far_ref[...].astype(BF16)
    copies = []
    for b in range(n // step):
        rows = slice(b * step, (b + 1) * step)
        base = top_ref[rows, :] if b * step < top else low_ref[b * step - top : (b + 1) * step - top, :]
        out_ref[rows, :] = (base + dot(ut_ref[rows, :], far)).astype(BF16)
        copies.append(pltpu.make_async_copy(out_ref.at[rows], out_hbm.at[rows], sems.at[b]))
        copies[-1].start()
    for copy in copies:
        copy.wait()


SMEM = pl.BlockSpec(memory_space=pltpu.SMEM)
VMEM = pl.BlockSpec(memory_space=pltpu.VMEM)
ANY = pl.BlockSpec(memory_space=pl.ANY)
HBM = pl.BlockSpec(memory_space=pltpu.HBM)


def grant(mib):
    return pltpu.CompilerParams(vmem_limit_bytes=mib << 20)


def in_hbm(*arrays):
    return [pltpu.with_memory_space_constraint(a, pltpu.HBM) for a in arrays]


def in_vmem(*arrays):
    return [pltpu.with_memory_space_constraint(a, pltpu.VMEM) for a in arrays]


def shape(dims, dtype=F32):
    return jax.ShapeDtypeStruct(dims, dtype)


def per_device(sources, tree_perm, leaf_blocks, u_factors, v_factors, level_ranks):
    n, rhs = sources.shape
    rank = u_factors.shape[1]
    half = 4 * rank
    low_rows = 768
    core = lax.axis_index("c").reshape(1)
    me = lax.axis_index(MIDDLE).reshape(1)
    perm = tree_perm.reshape(1, n)
    mine, send = pl.pallas_call(
        coef_kernel,
        name="coef",
        in_specs=[SMEM, HBM, HBM, HBM],
        out_specs=[VMEM, VMEM],
        out_shape=[shape((half, rhs)), shape((half + rank, rhs))],
        scratch_shapes=[
            pltpu.VMEM((rhs // 128, 2 * half, 128), F32),
            pltpu.VMEM((1, n), jnp.int32),
            pltpu.VMEM((9, rank, n), BF16),
            pltpu.VMEM((n, rhs), BF16),
            pltpu.SemaphoreType.DMA,
            pltpu.SemaphoreType.DMA,
            pltpu.SemaphoreType.DMA((n // 256,)),
        ],
        compiler_params=grant(14),
    )(core, *in_hbm(perm, v_factors, sources))
    pair = lax.all_gather(send, "c")
    partial = pl.pallas_call(
        add_kernel,
        name="add",
        in_specs=[SMEM, SMEM, VMEM, VMEM],
        out_specs=VMEM,
        out_shape=pltpu.VMEM((half, rhs), F32),
        compiler_params=grant(4),
    )(core, me, *in_vmem(mine, pair)).reshape(8, 16, rhs)
    got = lax.all_to_all(partial, OUTER, 0, 0, tiled=True)
    rows, fine, token = pl.pallas_call(
        middle_kernel,
        name="middle",
        in_specs=[SMEM, VMEM],
        out_specs=[VMEM] * 3,
        out_shape=[shape((32, 2, rhs)), pltpu.VMEM((8, 8, rhs), F32), shape((8, 128))],
        compiler_params=grant(4),
    )(me, got)
    top, low, ut, token = pl.pallas_call(
        local_kernel,
        name="local",
        in_specs=[SMEM, SMEM, VMEM] + [HBM] * 4 + [VMEM, ANY],
        out_specs=[VMEM, HBM, VMEM, VMEM],
        out_shape=[
            pltpu.VMEM((n - low_rows, rhs), F32),
            pltpu.HBM((low_rows, rhs), F32),
            pltpu.VMEM((n, 2 * half), BF16),
            shape((8, 128)),
        ],
        scratch_shapes=[
            pltpu.VMEM((n, rhs), BF16),
            pltpu.VMEM(leaf_blocks.shape, BF16),
            pltpu.VMEM(u_factors.shape, BF16),
            pltpu.VMEM((rank, n), BF16),
            pltpu.VMEM((n, rhs), BF16),
            pltpu.VMEM((n // 128, 2 * half, 128), F32),
            pltpu.VMEM((2 * half, n), BF16),
            pltpu.VMEM((3 * rank, n), BF16),
            pltpu.VMEM((3 * rank, rhs), BF16),
            pltpu.VMEM((low_rows, rhs), F32),
            pltpu.SemaphoreType.DMA((2,)),
            pltpu.SemaphoreType.DMA((n // 256,)),
            pltpu.SemaphoreType.DMA((n // 256,)),
            pltpu.SemaphoreType.DMA((low_rows // 256,)),
        ],
        compiler_params=grant(12),
        cost_estimate=pl.CostEstimate(flops=4_700_000_000, bytes_accessed=8_000_000, transcendentals=0),
    )(level_ranks, core, *in_vmem(perm), *in_hbm(sources, leaf_blocks, u_factors, v_factors), *in_vmem(pair), token)
    rows = lax.all_to_all(rows, MIDDLE, 0, 0, tiled=True)
    far = pl.pallas_call(
        far_kernel,
        name="far",
        in_specs=[SMEM, VMEM, VMEM, ANY],
        out_specs=VMEM,
        out_shape=shape((8, 16, rhs)),
        scratch_shapes=[pltpu.VMEM((16, rhs), F32)],
        compiler_params=grant(4),
    )(me, rows, *in_vmem(fine), token)
    far = lax.all_to_all(far, OUTER, 0, 0, tiled=True)
    far = lax.all_gather(far.reshape(half, rhs), "c", axis=0, tiled=True)
    return pl.pallas_call(
        last_kernel,
        name="last",
        in_specs=[VMEM] * 4,
        out_specs=HBM,
        out_shape=pltpu.HBM((n, rhs), BF16),
        scratch_shapes=[
            pltpu.VMEM((n, rhs), BF16),
            pltpu.SemaphoreType.DMA((n // 128,)),
        ],
        compiler_params=grant(8),
    )(*in_vmem(far, ut, top, low))


def solution(mesh):
    torus = Mesh(mesh.devices.reshape(4, 4, 2, 2, 4, 2), AXES)
    placed = (P(AXES, None), P(AXES), P(AXES, None), P(None, None, AXES), P(None, None, AXES), P())
    return jax.shard_map(
        per_device, mesh=torus, in_specs=placed, out_specs=P(AXES, None), check_vma=False
    )
```

```python
import jax
import jax.numpy as jnp
from jax import lax
from jax.experimental import pallas as pl
from jax.experimental.pallas import tpu as pltpu
from jax.sharding import Mesh
from jax.sharding import PartitionSpec as P

AXES = ("y", "zh", "z1", "z0", "x", "c")
OUTER = ("z0", "x")
MIDDLE = ("y", "zh", "z1")
F32 = jnp.float32
BF16 = jnp.bfloat16
NN = (((1,), (0,)), ((), ()))
NT = (((1,), (1,)), ((), ()))


def dot(a, b, dims=NN):
    return lax.dot_general(a, b, dims, preferred_element_type=F32)


def one_hot_t(perm, first, count):
    n = perm.shape[1]
    j = lax.broadcasted_iota(jnp.int32, (count, n), 0) + first
    return jnp.where(j == perm, 1.0, 0.0).astype(BF16)


def coef_kernel(core, perm_hbm, v_hbm, s_hbm, mine_ref, send_ref, acc, perm_ref, v_ref, s_ref, perm_sem, v_sem, s_sem):
    n = s_ref.shape[0]
    levels, rank, _ = v_ref.shape
    step = 256
    perm_copy = pltpu.make_async_copy(perm_hbm, perm_ref, perm_sem)
    perm_copy.start()
    v_copy = pltpu.make_async_copy(v_hbm.at[0:levels], v_ref, v_sem)
    v_copy.start()

    def s_copy(k):
        rows = pl.ds(pl.multiple_of(k * step, step), step)
        return pltpu.make_async_copy(s_hbm.at[rows], s_ref.at[rows], s_sem.at[k])

    def start(k, _):
        s_copy(k).start()
        return 0

    lax.fori_loop(0, n // step, start, 0)
    perm_copy.wait()
    perm = perm_ref[...] & (n - 1)
    v_copy.wait()
    v = v_ref[...].reshape(levels * rank, n)
    vp = [dot(v, one_hot_t(perm, j, step), NT).astype(BF16) for j in range(0, n, step)]
    for k in range(n // step):
        s_copy(k).wait()
    total = dot(jnp.concatenate(vp, axis=1), s_ref[...])
    half = 4 * rank
    me = core[0]
    mine = pl.ds(pl.multiple_of(me * half, half), half)
    theirs = pl.ds(pl.multiple_of((1 - me) * half, half), half)
    for d in range(acc.shape[0]):
        lanes = slice(d * 128, (d + 1) * 128)
        for level in range(8):
            acc[d, pl.ds(level, rank, stride=8), :] = total[level * rank : (level + 1) * rank, lanes]
        mine_ref[:, lanes] = acc[d, mine, :]
        send_ref[0:half, lanes] = acc[d, theirs, :]
    send_ref[half : half + rank, :] = total[8 * rank : 9 * rank]


def add_kernel(core, _, mine_ref, pair_ref, out_ref):
    half = mine_ref.shape[0]
    out_ref[...] = mine_ref[...] + pair_ref[1 - core[0], 0:half, :]


def local_kernel(
    ranks, core, perm_ref, s_hbm, leaf_hbm, u_hbm, v_hbm, pair_ref, _,
    top_ref, low_hbm, ut_ref, token_ref,
    s_ref, leaf_ref, u_ref, v_ref, ord_ref, uf_ref, us_ref, ue_ref, fe_ref, low_ref, sems, s_sem, leaf_sem, low_sem,
):
    n, leaf = leaf_ref.shape
    rank = v_ref.shape[0]
    step = 256
    u_copy = pltpu.make_async_copy(u_hbm, u_ref, sems.at[0])
    v_copy = pltpu.make_async_copy(v_hbm.at[9], v_ref, sems.at[1])

    def s_copy(k):
        rows = pl.ds(pl.multiple_of(k * step, step), step)
        return pltpu.make_async_copy(s_hbm.at[rows], s_ref.at[rows], s_sem.at[k])

    def leaf_copy(k):
        rows = pl.ds(pl.multiple_of(k * step, step), step)
        return pltpu.make_async_copy(leaf_hbm.at[rows], leaf_ref.at[rows], leaf_sem.at[k])

    def start_s(k, _):
        s_copy(k).start()
        return 0

    def start_leaf(k, _):
        leaf_copy(k).start()
        return 0

    lax.fori_loop(0, n // step, start_s, 0)
    v_copy.start()
    u_copy.start()
    lax.fori_loop(0, n // step, start_leaf, 0)
    perm = perm_ref[...] & (n - 1)
    lane = lax.broadcasted_iota(jnp.int32, (128, 128), 1)

    def one_hot(i, count):
        hot = []
        for h in range(i, i + count, 128):
            column = jnp.broadcast_to(perm[:, h : h + 128], (128, 128)).T
            hot.append(
                jnp.concatenate(
                    [jnp.where(column == lane + j, 1.0, 0.0).astype(BF16) for j in range(0, n, 128)], axis=1
                )
            )
        return jnp.concatenate(hot, axis=0)

    tall = 512
    hot = one_hot(0, tall)
    for k in range(n // step):
        s_copy(k).wait()
    for i in range(0, n, tall):
        ord_ref[i : i + tall, :] = dot(hot, s_ref[...]).astype(BF16)
        if i + tall < n:
            hot = one_hot(i + tall, tall)
    u_copy.wait()
    row = lax.broadcasted_iota(jnp.int32, (rank, n), 0)
    lane_n = lax.broadcasted_iota(jnp.int32, (rank, n), 1)
    for level in range(8):
        kept = jnp.where(row < ranks[level], u_ref[level].astype(F32), 0.0)
        for d in range(n // 128):
            uf_ref[d, pl.ds(level, rank, stride=8), :] = kept[:, d * 128 : (d + 1) * 128]
    for d in range(n // 128):
        us_ref[:, d * 128 : (d + 1) * 128] = uf_ref[d].astype(BF16)
    ue_ref[0:rank, :] = jnp.where(row < ranks[8], u_ref[8].astype(F32), 0.0).astype(BF16)
    last = jnp.where(row < ranks[9], u_ref[9].astype(F32), 0.0)
    ue_ref[rank : 2 * rank, :] = jnp.where(lane_n < leaf, last, 0.0).astype(BF16)
    ue_ref[2 * rank : 3 * rank, :] = jnp.where(lane_n < leaf, 0.0, last).astype(BF16)

    v_copy.wait()
    for k in range(n // step):
        leaf_copy(k).wait()
    fe_ref[0:rank, :] = pair_ref[1 - core[0], 4 * rank :, :].astype(BF16)
    fe_ref[rank : 2 * rank, :] = dot(v_ref[:, leaf:], ord_ref[leaf:, :]).astype(BF16)
    fe_ref[2 * rank : 3 * rank, :] = dot(v_ref[:, :leaf], ord_ref[:leaf, :]).astype(BF16)
    top = top_ref.shape[0]
    kept = []
    for j, count in ((256, 512), (768, 256), (0, 256)):
        rows = slice(j, j + count)
        hot = one_hot_t(perm, j, count)
        leaves = [dot(hot[:, g : g + leaf], leaf_ref[g : g + leaf, :]).astype(BF16) for g in range(0, n, leaf)]
        ut_ref[rows, :] = dot(hot, us_ref[...], NT).astype(BF16)
        et = dot(hot, ue_ref[...], NT).astype(BF16)
        base = dot(jnp.concatenate(leaves, axis=1), ord_ref[...]) + dot(et, fe_ref[...])
        if j < top:
            top_ref[rows, :] = base
        else:
            part = slice(j - top, j - top + count)
            low_ref[part, :] = base
            kept.append(pltpu.make_async_copy(low_ref.at[part], low_hbm.at[part], low_sem.at[len(kept)]))
            kept[-1].start()
    token_ref[...] = jnp.zeros_like(token_ref)
    for copy in kept:
        copy.wait()


def level_at(apart):
    for bit, row in ((16, 0), (8, 1), (4, 2), (2, 3)):
        if apart & bit:
            return row
    return 4


def middle_kernel(me, got_ref, out_ref, fine_ref, token_ref):
    token_ref[...] = jnp.zeros_like(token_ref)
    rows = got_ref.shape[1]
    got = lambda z, x: got_ref[z * 4 + x]
    sums = [(got(z, 0) + got(z, 1)) + (got(z, 2) + got(z, 3)) for z in range(2)]
    total = sums[0] + sums[1]
    for z in range(2):
        for x in range(4):
            for j in range(rows // 8):
                at = lambda a, row: a[j * 8 + row : j * 8 + row + 1]
                fine_ref[z * 4 + x, j * 4 : j * 4 + 1, :] = at(sums[z ^ 1], 5)
                fine_ref[z * 4 + x, j * 4 + 1 : j * 4 + 2, :] = at(got(z, x ^ 2), 6) + at(got(z, x ^ 3), 6)
                fine_ref[z * 4 + x, j * 4 + 2 : j * 4 + 3, :] = at(got(z, x ^ 1), 7)
    for row in range(5):
        sent = jnp.concatenate([total[r + row : r + row + 1] for r in range(0, rows, 8)], axis=0)
        for apart in range(out_ref.shape[0]):
            if level_at(apart) == row:
                out_ref[me[0] ^ apart] = sent


def far_kernel(me, got_ref, fine_ref, _, out_ref, acc):
    rows = acc.shape[0]
    acc[...] = jnp.zeros_like(acc)
    for row in range(5):
        parts = [got_ref[me[0] ^ k] for k in range(1, got_ref.shape[0]) if level_at(k) == row]
        while len(parts) > 1:
            parts = [sum(parts[k : k + 2]) for k in range(0, len(parts), 2)]
        for j in range(rows // 8):
            acc[j * 8 + row : j * 8 + row + 1, :] = parts[0][j : j + 1]
    far = acc[...]
    for p in range(out_ref.shape[0]):
        out_ref[p] = far
        for j in range(rows // 8):
            out_ref[p, j * 8 + 5 : j * 8 + 8, :] = fine_ref[p, j * 4 : j * 4 + 3, :]


def last_kernel(far_ref, ut_ref, top_ref, low_ref, out_hbm, out_ref, sems):
    n, step = out_ref.shape[0], 128
    top = top_ref.shape[0]
    far = far_ref[...].astype(BF16)
    copies = []
    for b in range(n // step):
        rows = slice(b * step, (b + 1) * step)
        base = top_ref[rows, :] if b * step < top else low_ref[b * step - top : (b + 1) * step - top, :]
        out_ref[rows, :] = (base + dot(ut_ref[rows, :], far)).astype(BF16)
        copies.append(pltpu.make_async_copy(out_ref.at[rows], out_hbm.at[rows], sems.at[b]))
        copies[-1].start()
    for copy in copies:
        copy.wait()


SMEM = pl.BlockSpec(memory_space=pltpu.SMEM)
VMEM = pl.BlockSpec(memory_space=pltpu.VMEM)
ANY = pl.BlockSpec(memory_space=pl.ANY)
HBM = pl.BlockSpec(memory_space=pltpu.HBM)


def grant(mib):
    return pltpu.CompilerParams(vmem_limit_bytes=mib << 20)


def in_hbm(*arrays):
    return [pltpu.with_memory_space_constraint(a, pltpu.HBM) for a in arrays]


def in_vmem(*arrays):
    return [pltpu.with_memory_space_constraint(a, pltpu.VMEM) for a in arrays]


def shape(dims, dtype=F32):
    return jax.ShapeDtypeStruct(dims, dtype)


def per_device(sources, tree_perm, leaf_blocks, u_factors, v_factors, level_ranks):
    n, rhs = sources.shape
    rank = u_factors.shape[1]
    half = 4 * rank
    low_rows = 768
    core = lax.axis_index("c").reshape(1)
    me = lax.axis_index(MIDDLE).reshape(1)
    perm = tree_perm.reshape(1, n)
    mine, send = pl.pallas_call(
        coef_kernel,
        name="coef",
        in_specs=[SMEM, HBM, HBM, HBM],
        out_specs=[VMEM, VMEM],
        out_shape=[shape((half, rhs)), shape((half + rank, rhs))],
        scratch_shapes=[
            pltpu.VMEM((rhs // 128, 2 * half, 128), F32),
            pltpu.VMEM((1, n), jnp.int32),
            pltpu.VMEM((9, rank, n), BF16),
            pltpu.VMEM((n, rhs), BF16),
            pltpu.SemaphoreType.DMA,
            pltpu.SemaphoreType.DMA,
            pltpu.SemaphoreType.DMA((n // 256,)),
        ],
        compiler_params=grant(14),
    )(core, *in_hbm(perm, v_factors, sources))
    pair = lax.all_gather(send, "c")
    partial = pl.pallas_call(
        add_kernel,
        name="add",
        in_specs=[SMEM, SMEM, VMEM, VMEM],
        out_specs=VMEM,
        out_shape=pltpu.VMEM((half, rhs), F32),
        compiler_params=grant(4),
    )(core, me, *in_vmem(mine, pair)).reshape(8, 16, rhs)
    got = lax.all_to_all(partial, OUTER, 0, 0, tiled=True)
    rows, fine, token = pl.pallas_call(
        middle_kernel,
        name="middle",
        in_specs=[SMEM, VMEM],
        out_specs=[VMEM] * 3,
        out_shape=[shape((32, 2, rhs)), pltpu.VMEM((8, 8, rhs), F32), shape((8, 128))],
        compiler_params=grant(4),
    )(me, got)
    top, low, ut, token = pl.pallas_call(
        local_kernel,
        name="local",
        in_specs=[SMEM, SMEM, VMEM] + [HBM] * 4 + [VMEM, ANY],
        out_specs=[VMEM, HBM, VMEM, VMEM],
        out_shape=[
            pltpu.VMEM((n - low_rows, rhs), F32),
            pltpu.HBM((low_rows, rhs), F32),
            pltpu.VMEM((n, 2 * half), BF16),
            shape((8, 128)),
        ],
        scratch_shapes=[
            pltpu.VMEM((n, rhs), BF16),
            pltpu.VMEM(leaf_blocks.shape, BF16),
            pltpu.VMEM(u_factors.shape, BF16),
            pltpu.VMEM((rank, n), BF16),
            pltpu.VMEM((n, rhs), BF16),
            pltpu.VMEM((n // 128, 2 * half, 128), F32),
            pltpu.VMEM((2 * half, n), BF16),
            pltpu.VMEM((3 * rank, n), BF16),
            pltpu.VMEM((3 * rank, rhs), BF16),
            pltpu.VMEM((low_rows, rhs), F32),
            pltpu.SemaphoreType.DMA((2,)),
            pltpu.SemaphoreType.DMA((n // 256,)),
            pltpu.SemaphoreType.DMA((n // 256,)),
            pltpu.SemaphoreType.DMA((low_rows // 256,)),
        ],
        compiler_params=grant(12),
        cost_estimate=pl.CostEstimate(flops=4_700_000_000, bytes_accessed=8_000_000, transcendentals=0),
    )(level_ranks, core, *in_vmem(perm), *in_hbm(sources, leaf_blocks, u_factors, v_factors), *in_vmem(pair), token)
    rows = lax.all_to_all(rows, MIDDLE, 0, 0, tiled=True)
    far = pl.pallas_call(
        far_kernel,
        name="far",
        in_specs=[SMEM, VMEM, VMEM, ANY],
        out_specs=VMEM,
        out_shape=shape((8, 16, rhs)),
        scratch_shapes=[pltpu.VMEM((16, rhs), F32)],
        compiler_params=grant(4),
    )(me, rows, *in_vmem(fine), token)
    far = lax.all_to_all(far, OUTER, 0, 0, tiled=True)
    far = lax.all_gather(far.reshape(half, rhs), "c", axis=0, tiled=True)
    return pl.pallas_call(
        last_kernel,
        name="last",
        in_specs=[VMEM] * 4,
        out_specs=HBM,
        out_shape=pltpu.HBM((n, rhs), BF16),
        scratch_shapes=[
            pltpu.VMEM((n, rhs), BF16),
            pltpu.SemaphoreType.DMA((n // 128,)),
        ],
        compiler_params=grant(8),
    )(*in_vmem(far, ut, top, low))


def solution(mesh):
    torus = Mesh(mesh.devices.reshape(4, 4, 2, 2, 4, 2), AXES)
    placed = (P(AXES, None), P(AXES), P(AXES, None), P(None, None, AXES), P(None, None, AXES), P())
    return jax.shard_map(
        per_device, mesh=torus, in_specs=placed, out_specs=P(AXES, None), check_vma=False
    )
```

```python
import jax
import jax.numpy as jnp
from jax import lax
from jax.experimental import pallas as pl
from jax.experimental.pallas import tpu as pltpu
from jax.sharding import Mesh
from jax.sharding import PartitionSpec as P

AXES = ("y", "zh", "z1", "z0", "x", "c")
OUTER = ("z0", "x")
MIDDLE = ("z1", "y", "zh")
F32 = jnp.float32
BF16 = jnp.bfloat16
NN = (((1,), (0,)), ((), ()))
NT = (((1,), (1,)), ((), ()))


def dot(a, b, dims=NN):
    return lax.dot_general(a, b, dims, preferred_element_type=F32)


def one_hot_t(perm, first, count):
    n = perm.shape[1]
    j = lax.broadcasted_iota(jnp.int32, (count, n), 0) + first
    return jnp.where(j == perm, 1.0, 0.0).astype(BF16)


def coef_kernel(core, perm_hbm, v_hbm, s_hbm, mine_ref, send_ref, acc, perm_ref, v_ref, s_ref, perm_sem, v_sem, s_sem):
    n = s_ref.shape[0]
    levels, rank, _ = v_ref.shape
    step = 256
    perm_copy = pltpu.make_async_copy(perm_hbm, perm_ref, perm_sem)
    perm_copy.start()
    v_copy = pltpu.make_async_copy(v_hbm.at[0:levels], v_ref, v_sem)
    v_copy.start()

    def s_copy(k):
        rows = pl.ds(pl.multiple_of(k * step, step), step)
        return pltpu.make_async_copy(s_hbm.at[rows], s_ref.at[rows], s_sem.at[k])

    def start(k, _):
        s_copy(k).start()
        return 0

    lax.fori_loop(0, n // step, start, 0)
    perm_copy.wait()
    perm = perm_ref[...] & (n - 1)
    v_copy.wait()
    v = v_ref[...].reshape(levels * rank, n)
    vp = [dot(v, one_hot_t(perm, j, step), NT).astype(BF16) for j in range(0, n, step)]
    for k in range(n // step):
        s_copy(k).wait()
    total = dot(jnp.concatenate(vp, axis=1), s_ref[...])
    half = 4 * rank
    me = core[0]
    mine = pl.ds(pl.multiple_of(me * half, half), half)
    theirs = pl.ds(pl.multiple_of((1 - me) * half, half), half)
    for d in range(acc.shape[0]):
        lanes = slice(d * 128, (d + 1) * 128)
        for level in range(8):
            acc[d, pl.ds(level, rank, stride=8), :] = total[level * rank : (level + 1) * rank, lanes]
        mine_ref[:, lanes] = acc[d, mine, :]
        send_ref[0:half, lanes] = acc[d, theirs, :]
    send_ref[half : half + rank, :] = total[8 * rank : 9 * rank]


def add_kernel(core, _, mine_ref, pair_ref, out_ref):
    half = mine_ref.shape[0]
    out_ref[...] = mine_ref[...] + pair_ref[1 - core[0], 0:half, :]


def local_kernel(
    ranks, core, perm_ref, s_hbm, leaf_hbm, u_hbm, v_hbm, pair_ref, _,
    top_ref, low_hbm, ut_ref, token_ref,
    s_ref, leaf_ref, u_ref, v_ref, ord_ref, uf_ref, us_ref, ue_ref, fe_ref, low_ref, sems, s_sem, leaf_sem, low_sem,
):
    n, leaf = leaf_ref.shape
    rank = v_ref.shape[0]
    step = 256
    u_copy = pltpu.make_async_copy(u_hbm, u_ref, sems.at[0])
    v_copy = pltpu.make_async_copy(v_hbm.at[9], v_ref, sems.at[1])

    def s_copy(k):
        rows = pl.ds(pl.multiple_of(k * step, step), step)
        return pltpu.make_async_copy(s_hbm.at[rows], s_ref.at[rows], s_sem.at[k])

    def leaf_copy(k):
        rows = pl.ds(pl.multiple_of(k * step, step), step)
        return pltpu.make_async_copy(leaf_hbm.at[rows], leaf_ref.at[rows], leaf_sem.at[k])

    def start_s(k, _):
        s_copy(k).start()
        return 0

    def start_leaf(k, _):
        leaf_copy(k).start()
        return 0

    lax.fori_loop(0, n // step, start_s, 0)
    v_copy.start()
    u_copy.start()
    lax.fori_loop(0, n // step, start_leaf, 0)
    perm = perm_ref[...] & (n - 1)
    lane = lax.broadcasted_iota(jnp.int32, (128, 128), 1)

    def one_hot(i):
        hot = []
        for h in range(i, i + step, 128):
            column = jnp.broadcast_to(perm[:, h : h + 128], (128, 128)).T
            hot.append(
                jnp.concatenate(
                    [jnp.where(column == lane + j, 1.0, 0.0).astype(BF16) for j in range(0, n, 128)], axis=1
                )
            )
        return jnp.concatenate(hot, axis=0)

    hot = one_hot(0)
    for k in range(n // step):
        s_copy(k).wait()
    for i in range(0, n, step):
        ord_ref[i : i + step, :] = dot(hot, s_ref[...]).astype(BF16)
        if i + step < n:
            hot = one_hot(i + step)
    u_copy.wait()
    row = lax.broadcasted_iota(jnp.int32, (rank, n), 0)
    lane_n = lax.broadcasted_iota(jnp.int32, (rank, n), 1)
    for level in range(8):
        kept = jnp.where(row < ranks[level], u_ref[level].astype(F32), 0.0)
        for d in range(n // 128):
            uf_ref[d, pl.ds(level, rank, stride=8), :] = kept[:, d * 128 : (d + 1) * 128]
    for d in range(n // 128):
        us_ref[:, d * 128 : (d + 1) * 128] = uf_ref[d].astype(BF16)
    ue_ref[0:rank, :] = jnp.where(row < ranks[8], u_ref[8].astype(F32), 0.0).astype(BF16)
    last = jnp.where(row < ranks[9], u_ref[9].astype(F32), 0.0)
    ue_ref[rank : 2 * rank, :] = jnp.where(lane_n < leaf, last, 0.0).astype(BF16)
    ue_ref[2 * rank : 3 * rank, :] = jnp.where(lane_n < leaf, 0.0, last).astype(BF16)

    v_copy.wait()
    for k in range(n // step):
        leaf_copy(k).wait()
    fe_ref[0:rank, :] = pair_ref[1 - core[0], 4 * rank :, :].astype(BF16)
    fe_ref[rank : 2 * rank, :] = dot(v_ref[:, leaf:], ord_ref[leaf:, :]).astype(BF16)
    fe_ref[2 * rank : 3 * rank, :] = dot(v_ref[:, :leaf], ord_ref[:leaf, :]).astype(BF16)
    top = top_ref.shape[0]
    kept = []
    for j in [*range(top, n, step), *range(0, top, step)]:
        rows = slice(j, j + step)
        hot = one_hot_t(perm, j, step)
        leaves = [dot(hot[:, g : g + leaf], leaf_ref[g : g + leaf, :]).astype(BF16) for g in range(0, n, leaf)]
        ut_ref[rows, :] = dot(hot, us_ref[...], NT).astype(BF16)
        et = dot(hot, ue_ref[...], NT).astype(BF16)
        base = dot(jnp.concatenate(leaves, axis=1), ord_ref[...]) + dot(et, fe_ref[...])
        if j < top:
            top_ref[rows, :] = base
        else:
            part = slice(j - top, j - top + step)
            low_ref[part, :] = base
            kept.append(pltpu.make_async_copy(low_ref.at[part], low_hbm.at[part], low_sem.at[len(kept)]))
            kept[-1].start()
    token_ref[...] = jnp.zeros_like(token_ref)
    for copy in kept:
        copy.wait()


def level_at(apart):
    for bit, row in ((8, 0), (4, 1), (2, 2), (1, 3)):
        if apart & bit:
            return row
    return 4


def middle_kernel(me, got_ref, out_ref, fine_ref, token_ref):
    token_ref[...] = jnp.zeros_like(token_ref)
    rows = got_ref.shape[1]
    got = lambda z, x: got_ref[z * 4 + x]
    sums = [(got(z, 0) + got(z, 1)) + (got(z, 2) + got(z, 3)) for z in range(2)]
    total = sums[0] + sums[1]
    for z in range(2):
        for x in range(4):
            for j in range(rows // 8):
                at = lambda a, row: a[j * 8 + row : j * 8 + row + 1]
                fine_ref[z * 4 + x, j * 4 : j * 4 + 1, :] = at(sums[z ^ 1], 5)
                fine_ref[z * 4 + x, j * 4 + 1 : j * 4 + 2, :] = at(got(z, x ^ 2), 6) + at(got(z, x ^ 3), 6)
                fine_ref[z * 4 + x, j * 4 + 2 : j * 4 + 3, :] = at(got(z, x ^ 1), 7)
    for row in range(5):
        sent = jnp.concatenate([total[r + row : r + row + 1] for r in range(0, rows, 8)], axis=0)
        for apart in range(out_ref.shape[0]):
            if level_at(apart) == row:
                out_ref[me[0] ^ apart] = sent


def far_kernel(me, got_ref, fine_ref, _, out_ref, acc):
    rows = acc.shape[0]
    acc[...] = jnp.zeros_like(acc)
    for row in range(5):
        parts = [got_ref[me[0] ^ k] for k in range(1, got_ref.shape[0]) if level_at(k) == row]
        while len(parts) > 1:
            parts = [sum(parts[k : k + 2]) for k in range(0, len(parts), 2)]
        for j in range(rows // 8):
            acc[j * 8 + row : j * 8 + row + 1, :] = parts[0][j : j + 1]
    far = acc[...]
    for p in range(out_ref.shape[0]):
        out_ref[p] = far
        for j in range(rows // 8):
            out_ref[p, j * 8 + 5 : j * 8 + 8, :] = fine_ref[p, j * 4 : j * 4 + 3, :]


def last_kernel(far_ref, ut_ref, top_ref, low_ref, out_hbm, out_ref, sems):
    n, step = out_ref.shape[0], 128
    top = top_ref.shape[0]
    far = far_ref[...].astype(BF16)
    copies = []
    for b in range(n // step):
        rows = slice(b * step, (b + 1) * step)
        base = top_ref[rows, :] if b * step < top else low_ref[b * step - top : (b + 1) * step - top, :]
        out_ref[rows, :] = (base + dot(ut_ref[rows, :], far)).astype(BF16)
        copies.append(pltpu.make_async_copy(out_ref.at[rows], out_hbm.at[rows], sems.at[b]))
        copies[-1].start()
    for copy in copies:
        copy.wait()


SMEM = pl.BlockSpec(memory_space=pltpu.SMEM)
VMEM = pl.BlockSpec(memory_space=pltpu.VMEM)
ANY = pl.BlockSpec(memory_space=pl.ANY)
HBM = pl.BlockSpec(memory_space=pltpu.HBM)


def grant(mib):
    return pltpu.CompilerParams(vmem_limit_bytes=mib << 20)


def in_hbm(*arrays):
    return [pltpu.with_memory_space_constraint(a, pltpu.HBM) for a in arrays]


def in_vmem(*arrays):
    return [pltpu.with_memory_space_constraint(a, pltpu.VMEM) for a in arrays]


def shape(dims, dtype=F32):
    return jax.ShapeDtypeStruct(dims, dtype)


def per_device(sources, tree_perm, leaf_blocks, u_factors, v_factors, level_ranks):
    n, rhs = sources.shape
    rank = u_factors.shape[1]
    half = 4 * rank
    low_rows = 768
    core = lax.axis_index("c").reshape(1)
    me = lax.axis_index(MIDDLE).reshape(1)
    perm = tree_perm.reshape(1, n)
    mine, send = pl.pallas_call(
        coef_kernel,
        name="coef",
        in_specs=[SMEM, HBM, HBM, HBM],
        out_specs=[VMEM, VMEM],
        out_shape=[shape((half, rhs)), shape((half + rank, rhs))],
        scratch_shapes=[
            pltpu.VMEM((rhs // 128, 2 * half, 128), F32),
            pltpu.VMEM((1, n), jnp.int32),
            pltpu.VMEM((9, rank, n), BF16),
            pltpu.VMEM((n, rhs), BF16),
            pltpu.SemaphoreType.DMA,
            pltpu.SemaphoreType.DMA,
            pltpu.SemaphoreType.DMA((n // 256,)),
        ],
        compiler_params=grant(14),
    )(core, *in_hbm(perm, v_factors, sources))
    pair = lax.all_gather(send, "c")
    partial = pl.pallas_call(
        add_kernel,
        name="add",
        in_specs=[SMEM, SMEM, VMEM, VMEM],
        out_specs=VMEM,
        out_shape=pltpu.VMEM((half, rhs), F32),
        compiler_params=grant(4),
    )(core, me, *in_vmem(mine, pair)).reshape(8, 16, rhs)
    got = lax.all_to_all(partial, OUTER, 0, 0, tiled=True)
    rows, fine, token = pl.pallas_call(
        middle_kernel,
        name="middle",
        in_specs=[SMEM, VMEM],
        out_specs=[VMEM] * 3,
        out_shape=[shape((32, 2, rhs)), pltpu.VMEM((8, 8, rhs), F32), shape((8, 128))],
        compiler_params=grant(4),
    )(me, got)
    top, low, ut, token = pl.pallas_call(
        local_kernel,
        name="local",
        in_specs=[SMEM, SMEM, VMEM] + [HBM] * 4 + [VMEM, ANY],
        out_specs=[VMEM, HBM, VMEM, VMEM],
        out_shape=[
            pltpu.VMEM((n - low_rows, rhs), F32),
            pltpu.HBM((low_rows, rhs), F32),
            pltpu.VMEM((n, 2 * half), BF16),
            shape((8, 128)),
        ],
        scratch_shapes=[
            pltpu.VMEM((n, rhs), BF16),
            pltpu.VMEM(leaf_blocks.shape, BF16),
            pltpu.VMEM(u_factors.shape, BF16),
            pltpu.VMEM((rank, n), BF16),
            pltpu.VMEM((n, rhs), BF16),
            pltpu.VMEM((n // 128, 2 * half, 128), F32),
            pltpu.VMEM((2 * half, n), BF16),
            pltpu.VMEM((3 * rank, n), BF16),
            pltpu.VMEM((3 * rank, rhs), BF16),
            pltpu.VMEM((low_rows, rhs), F32),
            pltpu.SemaphoreType.DMA((2,)),
            pltpu.SemaphoreType.DMA((n // 256,)),
            pltpu.SemaphoreType.DMA((n // 256,)),
            pltpu.SemaphoreType.DMA((low_rows // 256,)),
        ],
        compiler_params=grant(12),
        cost_estimate=pl.CostEstimate(flops=4_700_000_000, bytes_accessed=8_000_000, transcendentals=0),
    )(level_ranks, core, *in_vmem(perm), *in_hbm(sources, leaf_blocks, u_factors, v_factors), *in_vmem(pair), token)
    rows = lax.all_to_all(rows, MIDDLE, 0, 0, tiled=True)
    far = pl.pallas_call(
        far_kernel,
        name="far",
        in_specs=[SMEM, VMEM, VMEM, ANY],
        out_specs=VMEM,
        out_shape=shape((8, 16, rhs)),
        scratch_shapes=[pltpu.VMEM((16, rhs), F32)],
        compiler_params=grant(4),
    )(me, rows, *in_vmem(fine), token)
    far = lax.all_to_all(far, OUTER, 0, 0, tiled=True)
    far = lax.all_gather(far.reshape(half, rhs), "c", axis=0, tiled=True)
    return pl.pallas_call(
        last_kernel,
        name="last",
        in_specs=[VMEM] * 4,
        out_specs=HBM,
        out_shape=pltpu.HBM((n, rhs), BF16),
        scratch_shapes=[
            pltpu.VMEM((n, rhs), BF16),
            pltpu.SemaphoreType.DMA((n // 128,)),
        ],
        compiler_params=grant(8),
    )(*in_vmem(far, ut, top, low))


def solution(mesh):
    torus = Mesh(mesh.devices.reshape(4, 4, 2, 2, 4, 2), AXES)
    placed = (P(AXES, None), P(AXES), P(AXES, None), P(None, None, AXES), P(None, None, AXES), P())
    return jax.shard_map(
        per_device, mesh=torus, in_specs=placed, out_specs=P(AXES, None), check_vma=False
    )
```

```python
import jax
import jax.numpy as jnp
from jax import lax
from jax.experimental import pallas as pl
from jax.experimental.pallas import tpu as pltpu
from jax.sharding import Mesh
from jax.sharding import PartitionSpec as P

AXES = ("y", "zh", "z1", "z0", "x", "c")
OUTER = ("x", "z0")
MIDDLE = ("y", "zh", "z1")
F32 = jnp.float32
BF16 = jnp.bfloat16
NN = (((1,), (0,)), ((), ()))
NT = (((1,), (1,)), ((), ()))


def dot(a, b, dims=NN):
    return lax.dot_general(a, b, dims, preferred_element_type=F32)


def one_hot_t(perm, first, count):
    n = perm.shape[1]
    j = lax.broadcasted_iota(jnp.int32, (count, n), 0) + first
    return jnp.where(j == perm, 1.0, 0.0).astype(BF16)


def coef_kernel(core, perm_hbm, v_hbm, s_hbm, mine_ref, send_ref, acc, perm_ref, v_ref, s_ref, perm_sem, v_sem, s_sem):
    n = s_ref.shape[0]
    levels, rank, _ = v_ref.shape
    step = 256
    perm_copy = pltpu.make_async_copy(perm_hbm, perm_ref, perm_sem)
    perm_copy.start()
    v_copy = pltpu.make_async_copy(v_hbm.at[0:levels], v_ref, v_sem)
    v_copy.start()

    def s_copy(k):
        rows = pl.ds(pl.multiple_of(k * step, step), step)
        return pltpu.make_async_copy(s_hbm.at[rows], s_ref.at[rows], s_sem.at[k])

    def start(k, _):
        s_copy(k).start()
        return 0

    lax.fori_loop(0, n // step, start, 0)
    perm_copy.wait()
    perm = perm_ref[...] & (n - 1)
    v_copy.wait()
    v = v_ref[...].reshape(levels * rank, n)
    vp = [dot(v, one_hot_t(perm, j, step), NT).astype(BF16) for j in range(0, n, step)]
    for k in range(n // step):
        s_copy(k).wait()
    total = dot(jnp.concatenate(vp, axis=1), s_ref[...])
    half = 4 * rank
    me = core[0]
    mine = pl.ds(pl.multiple_of(me * half, half), half)
    theirs = pl.ds(pl.multiple_of((1 - me) * half, half), half)
    for d in range(acc.shape[0]):
        lanes = slice(d * 128, (d + 1) * 128)
        for level in range(8):
            acc[d, pl.ds(level, rank, stride=8), :] = total[level * rank : (level + 1) * rank, lanes]
        mine_ref[:, lanes] = acc[d, mine, :]
        send_ref[0:half, lanes] = acc[d, theirs, :]
    send_ref[half : half + rank, :] = total[8 * rank : 9 * rank]


def add_kernel(core, _, mine_ref, pair_ref, out_ref):
    half = mine_ref.shape[0]
    out_ref[...] = mine_ref[...] + pair_ref[1 - core[0], 0:half, :]


def local_kernel(
    ranks, core, perm_ref, s_hbm, leaf_hbm, u_hbm, v_hbm, pair_ref, _,
    top_ref, low_hbm, ut_ref, token_ref,
    s_ref, leaf_ref, u_ref, v_ref, ord_ref, uf_ref, us_ref, ue_ref, fe_ref, low_ref, sems, s_sem, leaf_sem, low_sem,
):
    n, leaf = leaf_ref.shape
    rank = v_ref.shape[0]
    step = 256
    u_copy = pltpu.make_async_copy(u_hbm, u_ref, sems.at[0])
    v_copy = pltpu.make_async_copy(v_hbm.at[9], v_ref, sems.at[1])

    def s_copy(k):
        rows = pl.ds(pl.multiple_of(k * step, step), step)
        return pltpu.make_async_copy(s_hbm.at[rows], s_ref.at[rows], s_sem.at[k])

    def leaf_copy(k):
        rows = pl.ds(pl.multiple_of(k * step, step), step)
        return pltpu.make_async_copy(leaf_hbm.at[rows], leaf_ref.at[rows], leaf_sem.at[k])

    def start_s(k, _):
        s_copy(k).start()
        return 0

    def start_leaf(k, _):
        leaf_copy(k).start()
        return 0

    lax.fori_loop(0, n // step, start_s, 0)
    v_copy.start()
    u_copy.start()
    lax.fori_loop(0, n // step, start_leaf, 0)
    perm = perm_ref[...] & (n - 1)
    lane = lax.broadcasted_iota(jnp.int32, (128, 128), 1)

    def one_hot(i):
        hot = []
        for h in range(i, i + step, 128):
            column = jnp.broadcast_to(perm[:, h : h + 128], (128, 128)).T
            hot.append(
                jnp.concatenate(
                    [jnp.where(column == lane + j, 1.0, 0.0).astype(BF16) for j in range(0, n, 128)], axis=1
                )
            )
        return jnp.concatenate(hot, axis=0)

    hot = one_hot(0)
    for k in range(n // step):
        s_copy(k).wait()
    for i in range(0, n, step):
        ord_ref[i : i + step, :] = dot(hot, s_ref[...]).astype(BF16)
        if i + step < n:
            hot = one_hot(i + step)
    u_copy.wait()
    row = lax.broadcasted_iota(jnp.int32, (rank, n), 0)
    lane_n = lax.broadcasted_iota(jnp.int32, (rank, n), 1)
    for level in range(8):
        kept = jnp.where(row < ranks[level], u_ref[level].astype(F32), 0.0)
        for d in range(n // 128):
            uf_ref[d, pl.ds(level, rank, stride=8), :] = kept[:, d * 128 : (d + 1) * 128]
    for d in range(n // 128):
        us_ref[:, d * 128 : (d + 1) * 128] = uf_ref[d].astype(BF16)
    ue_ref[0:rank, :] = jnp.where(row < ranks[8], u_ref[8].astype(F32), 0.0).astype(BF16)
    last = jnp.where(row < ranks[9], u_ref[9].astype(F32), 0.0)
    ue_ref[rank : 2 * rank, :] = jnp.where(lane_n < leaf, last, 0.0).astype(BF16)
    ue_ref[2 * rank : 3 * rank, :] = jnp.where(lane_n < leaf, 0.0, last).astype(BF16)

    v_copy.wait()
    for k in range(n // step):
        leaf_copy(k).wait()
    fe_ref[0:rank, :] = pair_ref[1 - core[0], 4 * rank :, :].astype(BF16)
    fe_ref[rank : 2 * rank, :] = dot(v_ref[:, leaf:], ord_ref[leaf:, :]).astype(BF16)
    fe_ref[2 * rank : 3 * rank, :] = dot(v_ref[:, :leaf], ord_ref[:leaf, :]).astype(BF16)
    top = top_ref.shape[0]
    kept = []
    for j in [*range(top, n, step), *range(0, top, step)]:
        rows = slice(j, j + step)
        hot = one_hot_t(perm, j, step)
        leaves = [dot(hot[:, g : g + leaf], leaf_ref[g : g + leaf, :]).astype(BF16) for g in range(0, n, leaf)]
        ut_ref[rows, :] = dot(hot, us_ref[...], NT).astype(BF16)
        et = dot(hot, ue_ref[...], NT).astype(BF16)
        base = dot(jnp.concatenate(leaves, axis=1), ord_ref[...]) + dot(et, fe_ref[...])
        if j < top:
            top_ref[rows, :] = base
        else:
            part = slice(j - top, j - top + step)
            low_ref[part, :] = base
            kept.append(pltpu.make_async_copy(low_ref.at[part], low_hbm.at[part], low_sem.at[len(kept)]))
            kept[-1].start()
    token_ref[...] = jnp.zeros_like(token_ref)
    for copy in kept:
        copy.wait()


def level_at(apart):
    for bit, row in ((16, 0), (8, 1), (4, 2), (2, 3)):
        if apart & bit:
            return row
    return 4


def middle_kernel(me, got_ref, out_ref, fine_ref, token_ref):
    token_ref[...] = jnp.zeros_like(token_ref)
    rows = got_ref.shape[1]
    got = lambda z, x: got_ref[x * 2 + z]
    sums = [(got(z, 0) + got(z, 1)) + (got(z, 2) + got(z, 3)) for z in range(2)]
    total = sums[0] + sums[1]
    for z in range(2):
        for x in range(4):
            for j in range(rows // 8):
                at = lambda a, row: a[j * 8 + row : j * 8 + row + 1]
                fine_ref[x * 2 + z, j * 4 : j * 4 + 1, :] = at(sums[z ^ 1], 5)
                fine_ref[x * 2 + z, j * 4 + 1 : j * 4 + 2, :] = at(got(z, x ^ 2), 6) + at(got(z, x ^ 3), 6)
                fine_ref[x * 2 + z, j * 4 + 2 : j * 4 + 3, :] = at(got(z, x ^ 1), 7)
    for row in range(5):
        sent = jnp.concatenate([total[r + row : r + row + 1] for r in range(0, rows, 8)], axis=0)
        for apart in range(out_ref.shape[0]):
            if level_at(apart) == row:
                out_ref[me[0] ^ apart] = sent


def far_kernel(me, got_ref, fine_ref, _, out_ref, acc):
    rows = acc.shape[0]
    acc[...] = jnp.zeros_like(acc)
    for row in range(5):
        parts = [got_ref[me[0] ^ k] for k in range(1, got_ref.shape[0]) if level_at(k) == row]
        while len(parts) > 1:
            parts = [sum(parts[k : k + 2]) for k in range(0, len(parts), 2)]
        for j in range(rows // 8):
            acc[j * 8 + row : j * 8 + row + 1, :] = parts[0][j : j + 1]
    far = acc[...]
    for p in range(out_ref.shape[0]):
        out_ref[p] = far
        for j in range(rows // 8):
            out_ref[p, j * 8 + 5 : j * 8 + 8, :] = fine_ref[p, j * 4 : j * 4 + 3, :]


def last_kernel(far_ref, ut_ref, top_ref, low_ref, out_hbm, out_ref, sems):
    n, step = out_ref.shape[0], 128
    top = top_ref.shape[0]
    far = far_ref[...].astype(BF16)
    copies = []
    for b in range(n // step):
        rows = slice(b * step, (b + 1) * step)
        base = top_ref[rows, :] if b * step < top else low_ref[b * step - top : (b + 1) * step - top, :]
        out_ref[rows, :] = (base + dot(ut_ref[rows, :], far)).astype(BF16)
        copies.append(pltpu.make_async_copy(out_ref.at[rows], out_hbm.at[rows], sems.at[b]))
        copies[-1].start()
    for copy in copies:
        copy.wait()


SMEM = pl.BlockSpec(memory_space=pltpu.SMEM)
VMEM = pl.BlockSpec(memory_space=pltpu.VMEM)
ANY = pl.BlockSpec(memory_space=pl.ANY)
HBM = pl.BlockSpec(memory_space=pltpu.HBM)


def grant(mib):
    return pltpu.CompilerParams(vmem_limit_bytes=mib << 20)


def in_hbm(*arrays):
    return [pltpu.with_memory_space_constraint(a, pltpu.HBM) for a in arrays]


def in_vmem(*arrays):
    return [pltpu.with_memory_space_constraint(a, pltpu.VMEM) for a in arrays]


def shape(dims, dtype=F32):
    return jax.ShapeDtypeStruct(dims, dtype)


def per_device(sources, tree_perm, leaf_blocks, u_factors, v_factors, level_ranks):
    n, rhs = sources.shape
    rank = u_factors.shape[1]
    half = 4 * rank
    low_rows = 768
    core = lax.axis_index("c").reshape(1)
    me = lax.axis_index(MIDDLE).reshape(1)
    perm = tree_perm.reshape(1, n)
    mine, send = pl.pallas_call(
        coef_kernel,
        name="coef",
        in_specs=[SMEM, HBM, HBM, HBM],
        out_specs=[VMEM, VMEM],
        out_shape=[shape((half, rhs)), shape((half + rank, rhs))],
        scratch_shapes=[
            pltpu.VMEM((rhs // 128, 2 * half, 128), F32),
            pltpu.VMEM((1, n), jnp.int32),
            pltpu.VMEM((9, rank, n), BF16),
            pltpu.VMEM((n, rhs), BF16),
            pltpu.SemaphoreType.DMA,
            pltpu.SemaphoreType.DMA,
            pltpu.SemaphoreType.DMA((n // 256,)),
        ],
        compiler_params=grant(14),
    )(core, *in_hbm(perm, v_factors, sources))
    pair = lax.all_gather(send, "c")
    partial = pl.pallas_call(
        add_kernel,
        name="add",
        in_specs=[SMEM, SMEM, VMEM, VMEM],
        out_specs=VMEM,
        out_shape=pltpu.VMEM((half, rhs), F32),
        compiler_params=grant(4),
    )(core, me, *in_vmem(mine, pair)).reshape(8, 16, rhs)
    got = lax.all_to_all(partial, OUTER, 0, 0, tiled=True)
    rows, fine, token = pl.pallas_call(
        middle_kernel,
        name="middle",
        in_specs=[SMEM, VMEM],
        out_specs=[VMEM] * 3,
        out_shape=[shape((32, 2, rhs)), pltpu.VMEM((8, 8, rhs), F32), shape((8, 128))],
        compiler_params=grant(4),
    )(me, got)
    top, low, ut, token = pl.pallas_call(
        local_kernel,
        name="local",
        in_specs=[SMEM, SMEM, VMEM] + [HBM] * 4 + [VMEM, ANY],
        out_specs=[VMEM, HBM, VMEM, VMEM],
        out_shape=[
            pltpu.VMEM((n - low_rows, rhs), F32),
            pltpu.HBM((low_rows, rhs), F32),
            pltpu.VMEM((n, 2 * half), BF16),
            shape((8, 128)),
        ],
        scratch_shapes=[
            pltpu.VMEM((n, rhs), BF16),
            pltpu.VMEM(leaf_blocks.shape, BF16),
            pltpu.VMEM(u_factors.shape, BF16),
            pltpu.VMEM((rank, n), BF16),
            pltpu.VMEM((n, rhs), BF16),
            pltpu.VMEM((n // 128, 2 * half, 128), F32),
            pltpu.VMEM((2 * half, n), BF16),
            pltpu.VMEM((3 * rank, n), BF16),
            pltpu.VMEM((3 * rank, rhs), BF16),
            pltpu.VMEM((low_rows, rhs), F32),
            pltpu.SemaphoreType.DMA((2,)),
            pltpu.SemaphoreType.DMA((n // 256,)),
            pltpu.SemaphoreType.DMA((n // 256,)),
            pltpu.SemaphoreType.DMA((low_rows // 256,)),
        ],
        compiler_params=grant(12),
        cost_estimate=pl.CostEstimate(flops=4_700_000_000, bytes_accessed=8_000_000, transcendentals=0),
    )(level_ranks, core, *in_vmem(perm), *in_hbm(sources, leaf_blocks, u_factors, v_factors), *in_vmem(pair), token)
    rows = lax.all_to_all(rows, MIDDLE, 0, 0, tiled=True)
    far = pl.pallas_call(
        far_kernel,
        name="far",
        in_specs=[SMEM, VMEM, VMEM, ANY],
        out_specs=VMEM,
        out_shape=shape((8, 16, rhs)),
        scratch_shapes=[pltpu.VMEM((16, rhs), F32)],
        compiler_params=grant(4),
    )(me, rows, *in_vmem(fine), token)
    far = lax.all_to_all(far, OUTER, 0, 0, tiled=True)
    far = lax.all_gather(far.reshape(half, rhs), "c", axis=0, tiled=True)
    return pl.pallas_call(
        last_kernel,
        name="last",
        in_specs=[VMEM] * 4,
        out_specs=HBM,
        out_shape=pltpu.HBM((n, rhs), BF16),
        scratch_shapes=[
            pltpu.VMEM((n, rhs), BF16),
            pltpu.SemaphoreType.DMA((n // 128,)),
        ],
        compiler_params=grant(8),
    )(*in_vmem(far, ut, top, low))


def solution(mesh):
    torus = Mesh(mesh.devices.reshape(4, 4, 2, 2, 4, 2), AXES)
    placed = (P(AXES, None), P(AXES), P(AXES, None), P(None, None, AXES), P(None, None, AXES), P())
    return jax.shard_map(
        per_device, mesh=torus, in_specs=placed, out_specs=P(AXES, None), check_vma=False
    )
```
